16 devices in a mesh: col: 2 (over z), row: 8 (over y, x, core).
Axes of the slice: x: 2, y: 2, z: 2, core: 2. Of those that a mesh axis runs over, the one named last changes fastest.
Arguments:
- inter_mask: int32 [8192, 32768], P('row', 'col')
- user_emb: bfloat16 [8192, 64], P(('row', 'col'))
- item_emb: bfloat16 [32768, 64], P(('col', 'row'))
- triples: int32 [8192, 3], replicated
Outputs:
- output 1: bfloat16 [8192, 64], P(('row', 'col'))
- output 2: bfloat16 [32768, 64], P(('col', 'row'))
- output 3: float32 [], replicated
- output 4: float32 [8192, 64], P(('row', 'col'))
- output 5: float32 [32768, 64], P(('col', 'row'))
All inputs are finite; a program needn't handle non-finite values.
Results may differ from the reference program's by a relative error of at most 0.00971148.
Values are sent between devices in bfloat16 or wider.
A program may use at most 1 GiB of HBM per device.

```python
import jax
import jax.numpy as jnp
from jax import lax

NUM_USERS = 8192
NUM_ITEMS = 32768
EMBED_DIM = 64
BATCH_SIZE = 8192
LAYERS = 3


def setup_inputs(seed: int = 0) -> dict:
    base_key = jax.random.key(seed)
    key_list = jax.random.split(base_key, 10)
    act_user = jax.random.randint(key_list[0], (NUM_USERS,), 1, 5)
    act_item = jax.random.randint(key_list[1], (NUM_ITEMS,), 1, 5)
    draw_vals = jax.random.randint(key_list[2], (NUM_USERS, NUM_ITEMS), 0, 2 * NUM_ITEMS)
    inter_mask = (draw_vals < act_user[:, None] * act_item[None, :] * 10).astype(jnp.int32)
    emb_scale = EMBED_DIM ** -0.25
    mean_user = jax.random.normal(key_list[3], (EMBED_DIM,), jnp.float32)
    mean_item = jax.random.normal(key_list[4], (EMBED_DIM,), jnp.float32)
    noise_user = jax.random.normal(key_list[5], (NUM_USERS, EMBED_DIM), jnp.float32)
    noise_item = jax.random.normal(key_list[6], (NUM_ITEMS, EMBED_DIM), jnp.float32)
    user_emb = ((mean_user[None, :] + noise_user) * emb_scale).astype(jnp.bfloat16)
    item_emb = ((mean_item[None, :] + noise_item) * emb_scale).astype(jnp.bfloat16)
    user_ids = jax.random.randint(key_list[7], (BATCH_SIZE,), 0, NUM_USERS)
    user_ids = user_ids.at[0].set(NUM_USERS - 1).at[1].set(0)
    pos_ids = jax.random.randint(key_list[8], (BATCH_SIZE,), 0, NUM_ITEMS)
    pos_ids = pos_ids.at[0].set(NUM_ITEMS - 1).at[1].set(0)
    neg_ids = jax.random.randint(key_list[9], (BATCH_SIZE,), 0, NUM_ITEMS)
    neg_ids = neg_ids.at[0].set(0).at[1].set(NUM_ITEMS - 1)
    triples = jnp.stack([user_ids, pos_ids, neg_ids], axis=1).astype(jnp.int32)
    return {'inter_mask': inter_mask, 'user_emb': user_emb, 'item_emb': item_emb, 'triples': triples}


def reference(inter_mask, user_emb, item_emb, triples):
    deg_user = jnp.maximum(jnp.sum(inter_mask, axis=1, dtype=jnp.int32), 1)
    deg_item = jnp.maximum(jnp.sum(inter_mask, axis=0, dtype=jnp.int32), 1)
    scale_user = lax.rsqrt(deg_user.astype(jnp.float32))
    scale_item = lax.rsqrt(deg_item.astype(jnp.float32))
    adj_mat = (scale_user[:, None] * inter_mask.astype(jnp.float32) * scale_item[None, :]).astype(jnp.bfloat16)

    def to_users(item_side):
        return jnp.dot(adj_mat, item_side, preferred_element_type=jnp.float32)

    def to_items(user_side):
        return lax.dot_general(adj_mat, user_side, (((0,), (0,)), ((), ())), preferred_element_type=jnp.float32)

    user_cur = user_emb
    item_cur = item_emb
    user_acc = user_emb.astype(jnp.float32)
    item_acc = item_emb.astype(jnp.float32)
    for _ in range(LAYERS):
        user_next = to_users(item_cur).astype(jnp.bfloat16)
        item_next = to_items(user_cur).astype(jnp.bfloat16)
        user_acc = user_acc + user_next.astype(jnp.float32)
        item_acc = item_acc + item_next.astype(jnp.float32)
        user_cur, item_cur = user_next, item_next
    user_out = (user_acc / (LAYERS + 1)).astype(jnp.bfloat16)
    item_out = (item_acc / (LAYERS + 1)).astype(jnp.bfloat16)

    def score_loss(user_table, item_table):
        e_user = jnp.take(user_table, triples[:, 0], axis=0)
        e_pos = jnp.take(item_table, triples[:, 1], axis=0)
        e_neg = jnp.take(item_table, triples[:, 2], axis=0)
        margin = jnp.sum(e_user * e_pos, axis=1) - jnp.sum(e_user * e_neg, axis=1)
        return jnp.mean(jax.nn.softplus(-margin))

    bpr_loss, pullback = jax.vjp(score_loss, user_out.astype(jnp.float32), item_out.astype(jnp.float32))
    grad_user_out, grad_item_out = pullback(jnp.ones_like(bpr_loss))
    src_user = grad_user_out / (LAYERS + 1)
    src_item = grad_item_out / (LAYERS + 1)
    cot_user = src_user.astype(jnp.bfloat16)
    cot_item = src_item.astype(jnp.bfloat16)
    for _ in range(LAYERS - 1):
        new_user = (src_user + to_users(cot_item)).astype(jnp.bfloat16)
        new_item = (src_item + to_items(cot_user)).astype(jnp.bfloat16)
        cot_user, cot_item = new_user, new_item
    grad_user = src_user + to_users(cot_item)
    grad_item = src_item + to_items(cot_user)
    return user_out, item_out, bpr_loss, grad_user, grad_item
```

```python
import functools

import jax
import jax.numpy as jnp
from jax import lax
from jax.experimental import pallas as pl
from jax.experimental.pallas import tpu as pltpu
from jax.sharding import PartitionSpec as P

LAYERS = 3
MESH = pl.DeviceIdType.MESH
F32 = jnp.float32
BF16 = jnp.bfloat16
VMEM_LIMIT = 66_000_000
NT = (((1,), (1,)), ((), ()))
CHUNK = 32


class Place:
    def __init__(self):
        r = lax.axis_index('row')
        c = lax.axis_index('col')
        core = r % 2
        x = (r // 2) % 2
        y = r // 4
        self.r, self.c, self.core = r, c, core
        self.mate = r + 1 - 2 * core
        self.xn = r + 2 - 4 * x
        self.yn = r + 4 - 8 * y
        self.dg = self.xn + 4 - 8 * y
        self.zc = 1 - c
        d = 1 - 2 * core
        self.mate_x, self.mate_y, self.mate_d = self.xn + d, self.yn + d, self.dg + d

    def to_row(self, src, dst, ssem, rsem, row):
        return pltpu.make_async_remote_copy(src_ref=src, dst_ref=dst, send_sem=ssem, recv_sem=rsem, device_id={'row': row}, device_id_type=MESH)

    def to_z(self, src, dst, ssem, rsem):
        return pltpu.make_async_remote_copy(src_ref=src, dst_ref=dst, send_sem=ssem, recv_sem=rsem, device_id={'col': self.zc}, device_id_type=MESH)


def entry_barrier(pc):
    bar = pltpu.get_barrier_semaphore()
    for j in range(1, 8):
        pl.semaphore_signal(bar, inc=1, device_id={'row': (pc.r + j) % 8}, device_id_type=MESH)
    pl.semaphore_signal(bar, inc=1, device_id={'col': pc.zc}, device_id_type=MESH)
    pl.semaphore_wait(bar, 8)


class Gather:
    def __init__(self, pc, xi, ssem, rsem):
        self.pc, self.xi, self.ssem, self.rsem = pc, xi, ssem, rsem
        self.sent = []

    def _send(self, k, ref, row):
        cp = self.pc.to_row(ref, ref, self.ssem.at[k], self.rsem.at[k], row)
        cp.start()
        self.sent.append(cp)

    def _recv(self, k, ref):
        self.pc.to_row(ref, ref, self.ssem.at[k], self.rsem.at[k], self.pc.mate).wait_recv()

    def start(self):
        pc, xi = self.pc, self.xi
        own = xi.at[pc.r]
        self._send(0, own, pc.xn)
        self._send(1, own, pc.yn)
        self._send(2, own, pc.mate)

    def wait_mate(self):
        self._recv(2, self.xi.at[self.pc.mate])

    def relay(self):
        pc, xi = self.pc, self.xi
        self._recv(0, xi.at[pc.xn])
        self._send(3, xi.at[pc.xn, 0:32], pc.yn)
        self._send(5, xi.at[pc.xn], pc.mate)
        self._recv(1, xi.at[pc.yn])
        self._send(4, xi.at[pc.yn, 32:64], pc.xn)
        self._send(6, xi.at[pc.yn], pc.mate)

    def wait_mates(self):
        pc, xi = self.pc, self.xi
        self._recv(5, xi.at[pc.mate_x])
        self._recv(6, xi.at[pc.mate_y])

    def last(self):
        pc, xi = self.pc, self.xi
        self._recv(3, xi.at[pc.dg, 0:32])
        self._recv(4, xi.at[pc.dg, 32:64])
        self._send(7, xi.at[pc.dg], pc.mate)

    def finish(self):
        self._recv(7, self.xi.at[self.pc.mate_d])
        for cp in self.sent:
            cp.wait_send()
        self.sent = []


class Scatter:
    def __init__(self, pc, pi, rd, rx, ry, rz, ssem, rsem):
        self.pc, self.pi, self.rd, self.rx, self.ry, self.rz = pc, pi, rd, rx, ry, rz
        self.ssem, self.rsem = ssem, rsem
        self.sent = []

    def _send(self, k, src, dst, row):
        cp = self.pc.to_row(src, dst, self.ssem.at[k], self.rsem.at[k], row)
        cp.start()
        self.sent.append(cp)

    def _recv(self, k, ref):
        self.pc.to_row(ref, ref, self.ssem.at[k], self.rsem.at[k], self.pc.mate).wait_recv()

    def send_mate(self):
        pc = self.pc
        for k, q in enumerate((pc.mate_d, pc.mate_x, pc.mate_y, pc.mate)):
            self._send(k, self.pi.at[q], self.rd.at[k], pc.mate)

    def first(self):
        pc, pi, rd = self.pc, self.pi, self.rd
        self._recv(0, rd.at[0])
        pi[pc.dg] += rd[0]
        self._send(4, pi.at[pc.dg, 0:32], self.rx.at[1], pc.xn)
        self._send(5, pi.at[pc.dg, 32:64], self.ry.at[1], pc.yn)
        self._recv(1, rd.at[1])
        pi[pc.xn] += rd[1]
        self._send(6, pi.at[pc.xn, 0:32], self.rx.at[0], pc.xn)
        self._recv(2, rd.at[2])
        pi[pc.yn] += rd[2]
        self._send(7, pi.at[pc.yn, 32:64], self.ry.at[0], pc.yn)
        self._recv(3, rd.at[3])
        pi[pc.r] += rd[3]

    def second(self):
        pc, pi = self.pc, self.pi
        self._recv(4, self.rx.at[1])
        pi[pc.yn, 0:32] += self.rx[1]
        self._send(8, pi.at[pc.yn, 0:32], self.rz.at[0], pc.yn)
        self._recv(5, self.ry.at[1])
        pi[pc.xn, 32:64] += self.ry[1]
        self._send(9, pi.at[pc.xn, 32:64], self.rz.at[1], pc.xn)

    def result(self, emit):
        pc, pi = self.pc, self.pi
        self._recv(6, self.rx.at[0])
        self._recv(7, self.ry.at[0])
        self._recv(8, self.rz.at[0])
        emit(0, pi[pc.r, 0:32] + self.rx[0] + self.rz[0])
        self._recv(9, self.rz.at[1])
        emit(1, pi[pc.r, 32:64] + self.ry[0] + self.rz[1])
        for cp in self.sent:
            cp.wait_send()
        self.sent = []


def item_part(a, xu, pi, parity):
    x = jnp.concatenate([xu[0], xu[1]], axis=1)

    def body(j, _):
        q = 2 * j + parity
        for n in range(0, 2048, 512):
            pi[q, :, n:n + 512] = jnp.dot(x, a[q, :, n:n + 512], preferred_element_type=F32)
        return 0

    lax.fori_loop(0, 4, body, 0)


def user_part(a, xi, up, shards, first):
    if first:
        up[...] = jnp.zeros_like(up)
    for q in shards:
        for h in range(2):
            up[h] += lax.dot_general(xi[q], a[q, h * 512:(h + 1) * 512, :], NT, preferred_element_type=F32)


def propagate(pc, a, xis, xus, ups, urs, scat, gath, zs, zr, fin_u, fin_i):
    me = pc

    def z_send(ch):
        cp = me.to_z(ups[ch].at[me.zc], urs[ch], zs.at[ch, 0], zr.at[ch, 0])
        cp.start()
        return cp

    def z_sum(ch, cp):
        cp.wait()
        return ups[ch][me.c] + urs[ch][...]

    def z_share(ch, xu):
        cp = me.to_z(xu.at[me.c], xu.at[me.c], zs.at[ch, 1], zr.at[ch, 1])
        cp.start()
        return cp

    sp, sq = scat
    gp, gq = gath
    other = 1 - me.core

    item_part(a, xus[0], sq.pi, other)
    sq.send_mate()
    item_part(a, xus[0], sq.pi, me.core)
    user_part(a, xis[0], ups[0], (me.r, me.xn), True)
    sq.first()
    user_part(a, xis[0], ups[0], (me.yn, me.mate, me.mate_x, me.mate_y, me.dg, me.mate_d), False)
    cp = z_send(0)
    u1 = z_sum(0, cp)
    xus[1][me.c] = fin_u(1, u1)
    cp = z_share(0, xus[1])
    cp.wait()
    item_part(a, xus[1], sp.pi, other)
    sp.send_mate()
    sq.second()
    item_part(a, xus[1], sp.pi, me.core)

    def keep1(half, value):
        xis[1][me.r, half * 32:half * 32 + 32] = fin_i(1, half, value)

    sq.result(keep1)
    gq.start()
    user_part(a, xis[1], ups[1], (me.r,), True)
    gq.relay()
    sp.first()
    gq.wait_mate()
    user_part(a, xis[1], ups[1], (me.xn, me.yn, me.mate), False)
    gq.last()
    gq.wait_mates()
    user_part(a, xis[1], ups[1], (me.mate_x, me.mate_y, me.dg), False)
    gq.finish()
    user_part(a, xis[1], ups[1], (me.mate_d,), False)
    cp = z_send(1)
    u2 = z_sum(1, cp)
    xus[2][me.c] = fin_u(2, u2)
    cp = z_share(1, xus[2])
    cp.wait()
    item_part(a, xus[2], sq.pi, other)
    sq.send_mate()
    sp.second()
    item_part(a, xus[2], sq.pi, me.core)
    sq.first()

    def keep2(half, value):
        xis[0][me.r, half * 32:half * 32 + 32] = fin_i(2, half, value)

    sp.result(keep2)
    gp.start()
    user_part(a, xis[0], ups[0], (me.r,), True)
    gp.relay()
    gp.wait_mate()
    user_part(a, xis[0], ups[0], (me.xn, me.yn, me.mate), False)
    sq.second()
    gp.last()
    gp.wait_mates()
    user_part(a, xis[0], ups[0], (me.mate_x, me.mate_y, me.dg), False)
    gp.finish()
    user_part(a, xis[0], ups[0], (me.mate_d,), False)
    cp = z_send(0)
    u3 = z_sum(0, cp)
    fin_u(3, u3)

    def keep3(half, value):
        fin_i(3, half, value)

    sq.result(keep3)


def comm_scratch():
    dma = pltpu.SemaphoreType.DMA
    return [
        pltpu.VMEM((8, 1024, 2048), BF16),
        pltpu.VMEM((2, 8, 64, 2048), BF16),
        pltpu.VMEM((3, 2, 64, 512), BF16),
        pltpu.VMEM((2, 2, 64, 512), F32),
        pltpu.VMEM((2, 64, 512), F32),
        pltpu.VMEM((2, 8, 64, 2048), F32),
        pltpu.VMEM((2, 4, 64, 2048), F32),
        pltpu.VMEM((2, 6, 32, 2048), F32),
        dma((2, 8)), dma((2, 8)), dma((2, 10)), dma((2, 10)), dma((2, 2)), dma((2, 2)),
    ]


def comm_objects(pc, a, xi, xu, up, ur, pi, rd, rxyz, gs, gr, ss, sr, zs, zr):
    scat = [Scatter(pc, pi.at[k], rd.at[k], rxyz.at[k, 0:2], rxyz.at[k, 2:4], rxyz.at[k, 4:6], ss.at[k], sr.at[k]) for k in range(2)]
    gath = [Gather(pc, xi.at[k], gs.at[k], gr.at[k]) for k in range(2)]
    return dict(pc=pc, a=a, xis=[xi.at[0], xi.at[1]], xus=[xu.at[k] for k in range(3)], ups=[up.at[0], up.at[1]],
                urs=[ur.at[0], ur.at[1]], scat=scat, gath=gath, zs=zs, zr=zr)


def forward_kernel(m_hbm, u0, i0, eu, ei, a_hbm, *scratch):
    comm, (stage, rowacc, cacc, dpi, drecv, dfull, du, dur, su, accu, acci, msem, ds, dr, osem) = scratch[:14], scratch[14:]
    pc = Place()
    objs = comm_objects(pc, *comm)
    a, xi, xu = comm[0], comm[1], comm[2]
    zs, zr = comm[12], comm[13]

    def fetch(i):
        return pltpu.make_async_copy(m_hbm.at[pl.ds(pl.multiple_of(i * CHUNK, CHUNK), CHUNK), :], stage.at[i % 3], msem.at[i % 3])

    n_chunk = 1024 // CHUNK
    for i in range(3):
        fetch(i).start()
    xi[0, pc.r] = i0[...]
    xu[0, pc.c] = u0[...]
    accu[...] = u0[...].astype(F32)
    acci[...] = i0[...].astype(F32)
    cacc[...] = jnp.zeros_like(cacc)
    entry_barrier(pc)
    gp = objs['gath'][0]
    gp.start()
    share0 = pc.to_z(xu.at[0, pc.c], xu.at[0, pc.c], zs.at[0, 1], zr.at[0, 1])
    share0.start()

    def chunk(i, _):
        slot = i % 3
        fetch(i).wait()
        rows = pl.ds(pl.multiple_of(i * CHUNK, CHUNK), CHUNK)

        def shard(q, racc):
            for n in range(0, 2048, 512):
                m = stage[slot, :, pl.ds(pl.multiple_of(q * 2048 + n, 512), 512)]
                a[q, rows, n:n + 512] = m.astype(F32).astype(BF16)
                cacc[q, :, n:n + 512] += m[0:8] + m[8:16] + m[16:24] + m[24:32]
                racc = racc + ((m[:, 0:128] + m[:, 128:256]) + (m[:, 256:384] + m[:, 384:512]))
            return racc

        rowacc[rows, :] = lax.fori_loop(0, 8, shard, jnp.zeros((CHUNK, 128), jnp.int32))

        @pl.when(i + 3 < n_chunk)
        def _():
            fetch(i + 3).start()

        return 0

    lax.fori_loop(0, 12, chunk, 0)
    gp.relay()
    lax.fori_loop(12, 20, chunk, 0)
    gp.last()
    gp.wait_mate()
    gp.wait_mates()
    lax.fori_loop(20, n_chunk, chunk, 0)
    gp.finish()
    share0.wait()

    def fold(q, _):
        t = jnp.sum(cacc[q], axis=0, keepdims=True)
        for s in range(8):
            dpi[q, s:s + 1, :] = t[:, s * 256:(s + 1) * 256]
        return 0

    lax.fori_loop(0, 8, fold, 0)
    copies = []
    for j in range(1, 8):
        p = (pc.r + j) % 8
        copies.append(pc.to_row(dpi.at[p], drecv.at[j - 1], ds.at[0, j - 1], dr.at[0, j - 1], p))
        copies[-1].start()
    rt = jnp.sum(rowacc[...].astype(F32).T, axis=0, keepdims=True)
    du[...] = jnp.broadcast_to(rt, (8, 1024)).astype(jnp.int32)
    zc = pc.to_z(du, dur, ds.at[0, 7], dr.at[0, 7])
    zc.start()
    total = dpi[pc.r]
    for j in range(1, 8):
        copies[j - 1].wait_recv()
        total = total + drecv[j - 1]
    dfull[pc.r] = total
    back = []
    for j in range(1, 8):
        p = (pc.r + j) % 8
        back.append(pc.to_row(dfull.at[pc.r], dfull.at[pc.r], ds.at[1, j - 1], dr.at[1, j - 1], p))
        back[-1].start()
    zc.wait_recv()
    s8 = lax.rsqrt(jnp.maximum(du[...] + dur[...], 1).astype(F32))
    su[...] = jnp.broadcast_to(s8[0:1], (128, 1024)).T
    for cp in back:
        cp.wait_recv()
    for cp in copies + back + [zc]:
        cp.wait_send()

    def form(q, _):
        for s in range(8):
            si = lax.rsqrt(jnp.maximum(dfull[q, s:s + 1, :], 1).astype(F32))

            def rows_body(t, _, s=s, si=si):
                rows = pl.ds(pl.multiple_of(t * 128, 128), 128)
                sub = su[rows, :]
                scale = (jnp.concatenate([sub, sub], axis=1) * si).astype(BF16)
                a[q, rows, s * 256:(s + 1) * 256] = a[q, rows, s * 256:(s + 1) * 256] * scale
                return 0

            lax.fori_loop(0, 8, rows_body, 0)
        return 0

    lax.fori_loop(0, 8, form, 0)
    out = pltpu.make_async_copy(a, a_hbm, osem)
    out.start()

    def fin_u(k, total):
        nxt = total.astype(BF16)
        accu[...] += nxt.astype(F32)
        return nxt

    def fin_i(k, half, total):
        nxt = total.astype(BF16)
        acci[half * 32:half * 32 + 32] += nxt.astype(F32)
        return nxt

    propagate(fin_u=fin_u, fin_i=fin_i, **objs)
    eu[...] = (accu[...] / (LAYERS + 1)).astype(BF16)
    ei[...] = (acci[...] / (LAYERS + 1)).astype(BF16)
    out.wait()


def backward_kernel(a_hbm, src_u, src_i, gu, gi, *scratch):
    comm, (osem,) = scratch[:14], scratch[14:]
    pc = Place()
    objs = comm_objects(pc, *comm)
    a, xi, xu = comm[0], comm[1], comm[2]
    zs, zr = comm[12], comm[13]
    load = pltpu.make_async_copy(a_hbm, a, osem)
    load.start()
    xi[0, pc.r] = src_i[...].astype(BF16)
    xu[0, pc.c] = src_u[...].astype(BF16)
    entry_barrier(pc)
    gp = objs['gath'][0]
    gp.start()
    share0 = pc.to_z(xu.at[0, pc.c], xu.at[0, pc.c], zs.at[0, 1], zr.at[0, 1])
    share0.start()
    gp.relay()
    gp.last()
    gp.wait_mate()
    gp.wait_mates()
    gp.finish()
    share0.wait()
    load.wait()

    def fin_u(k, total):
        value = src_u[...] + total
        if k == LAYERS:
            gu[...] = value
        return value.astype(BF16)

    def fin_i(k, half, total):
        rows = slice(half * 32, half * 32 + 32)
        value = src_i[rows] + total
        if k == LAYERS:
            gi[rows] = value
        return value.astype(BF16)

    propagate(fin_u=fin_u, fin_i=fin_i, **objs)


def forward_call(mask_blk, u0, i0):
    dma = pltpu.SemaphoreType.DMA
    vm = pl.BlockSpec(memory_space=pltpu.VMEM)
    hbm = pl.BlockSpec(memory_space=pl.ANY)
    i32 = jnp.int32
    return pl.pallas_call(
        forward_kernel,
        name='forward_chains',
        out_shape=(jax.ShapeDtypeStruct((64, 512), BF16), jax.ShapeDtypeStruct((64, 2048), BF16), jax.ShapeDtypeStruct((8, 1024, 2048), BF16)),
        in_specs=[hbm, vm, vm],
        out_specs=(vm, vm, hbm),
        scratch_shapes=comm_scratch() + [
            pltpu.VMEM((3, CHUNK, 16384), i32),
            pltpu.VMEM((1024, 128), i32),
            pltpu.VMEM((8, 8, 2048), i32),
            pltpu.VMEM((8, 8, 256), i32),
            pltpu.VMEM((7, 8, 256), i32),
            pltpu.VMEM((8, 8, 256), i32),
            pltpu.VMEM((8, 1024), i32),
            pltpu.VMEM((8, 1024), i32),
            pltpu.VMEM((1024, 128), F32),
            pltpu.VMEM((64, 512), F32),
            pltpu.VMEM((64, 2048), F32),
            dma((3,)), dma((2, 8)), dma((2, 8)), dma,
        ],
        compiler_params=pltpu.CompilerParams(collective_id=0, has_side_effects=True, vmem_limit_bytes=VMEM_LIMIT),
    )(mask_blk, u0, i0)


def backward_call(a, src_u, src_i):
    dma = pltpu.SemaphoreType.DMA
    vm = pl.BlockSpec(memory_space=pltpu.VMEM)
    hbm = pl.BlockSpec(memory_space=pl.ANY)
    return pl.pallas_call(
        backward_kernel,
        name='backward_chains',
        out_shape=(jax.ShapeDtypeStruct((64, 512), F32), jax.ShapeDtypeStruct((64, 2048), F32)),
        in_specs=[hbm, vm, vm],
        out_specs=(vm, vm),
        scratch_shapes=comm_scratch() + [dma],
        compiler_params=pltpu.CompilerParams(collective_id=1, has_side_effects=True, vmem_limit_bytes=VMEM_LIMIT),
    )(a, src_u, src_i)


def solution(mesh):
    n_col = mesh.shape['col']
    n_row = mesh.shape['row']

    def local_fn(mask_blk, user_emb, item_emb, triples):
        row_idx = lax.axis_index('row')
        col_idx = lax.axis_index('col')
        user_rows = user_emb.shape[0]
        item_rows = item_emb.shape[0]
        n_batch = triples.shape[0]

        eu_t, ei_t, adj = forward_call(mask_blk, user_emb.T, item_emb.T)
        user_final, item_final = eu_t.T, ei_t.T

        user_base = (row_idx * n_col + col_idx) * user_rows
        item_base = (col_idx * n_row + row_idx) * item_rows
        local_user = triples[:, 0] - user_base
        local_pos = triples[:, 1] - item_base
        local_neg = triples[:, 2] - item_base

        def lookup_rows(emb_table, local_ids):
            is_owned = (local_ids >= 0) & (local_ids < emb_table.shape[0])
            picked = jnp.take(emb_table, jnp.clip(local_ids, 0, emb_table.shape[0] - 1), axis=0).astype(jnp.float32)
            seg_ids = jnp.where(is_owned, local_ids, emb_table.shape[0])
            return jnp.where(is_owned[:, None], picked, 0.0), seg_ids

        rows_user, seg_user = lookup_rows(user_final, local_user)
        rows_pos, seg_pos = lookup_rows(item_final, local_pos)
        rows_neg, seg_neg = lookup_rows(item_final, local_neg)
        fetched = lax.psum(jnp.concatenate([rows_user, rows_pos, rows_neg], axis=0), ('row', 'col'))
        e_user = fetched[:n_batch]
        e_pos = fetched[n_batch:2 * n_batch]
        e_neg = fetched[2 * n_batch:]
        margin = jnp.sum(e_user * e_pos, axis=1) - jnp.sum(e_user * e_neg, axis=1)
        bpr_loss = jnp.mean(jax.nn.softplus(-margin))
        loss_coef = -jax.nn.sigmoid(-margin) / n_batch
        grad_eu = loss_coef[:, None] * (e_pos - e_neg)
        grad_epos = loss_coef[:, None] * e_user
        seed_user = jax.ops.segment_sum(grad_eu, seg_user, num_segments=user_rows)
        seed_item = jax.ops.segment_sum(jnp.concatenate([grad_epos, -grad_epos], axis=0), jnp.concatenate([seg_pos, seg_neg], axis=0), num_segments=item_rows)

        src_user = seed_user / (LAYERS + 1)
        src_item = seed_item / (LAYERS + 1)
        gu_t, gi_t = backward_call(adj, src_user.T, src_item.T)
        return user_final, item_final, bpr_loss, gu_t.T, gi_t.T

    user_spec = P(('row', 'col'), None)
    item_spec = P(('col', 'row'), None)
    return jax.shard_map(local_fn, mesh=mesh, in_specs=(P('row', 'col'), user_spec, item_spec, P()), out_specs=(user_spec, item_spec, P(), user_spec, item_spec), check_vma=False)
```

```python
import functools

import jax
import jax.numpy as jnp
from jax import lax
from jax.experimental import pallas as pl
from jax.experimental.pallas import tpu as pltpu
from jax.sharding import PartitionSpec as P

LAYERS = 3
MESH = pl.DeviceIdType.MESH
F32 = jnp.float32
BF16 = jnp.bfloat16
VMEM_LIMIT = 67_043_328
NT = (((1,), (1,)), ((), ()))
NONE, ONE, TWO, THREE = range(4)
D = 64
HALF = D // 2
SHARD = 2048
USERS = 512
GROUP = 128
FOLD = 256
ROWS = 8
SLOTS = 4
BATCH = 8192
ITEMS = ROWS * SHARD
LO, HI = slice(0, HALF), slice(HALF, D)


def choose(j, values):
    out = values[-1]
    for k in range(len(values) - 1):
        out = jnp.where(j == k, values[k], out)
    return out


def window(k, size):
    return pl.ds(pl.multiple_of(k * size, size), size)


class Place:
    def __init__(self):
        r = lax.axis_index('row')
        c = lax.axis_index('col')
        core = r % 2
        x = (r // 2) % 2
        y = r // 4
        self.r, self.c, self.core = r, c, core
        self.mate = r + 1 - 2 * core
        self.xn = r + 2 - 4 * x
        self.yn = r + 4 - 8 * y
        self.dg = self.xn + 4 - 8 * y
        self.zc = 1 - c
        d = 1 - 2 * core
        self.mate_x, self.mate_y, self.mate_d = self.xn + d, self.yn + d, self.dg + d

    def to_row(self, src, dst, ssem, rsem, row):
        return pltpu.make_async_remote_copy(src_ref=src, dst_ref=dst, send_sem=ssem, recv_sem=rsem, device_id={'row': row}, device_id_type=MESH)

    def to_z(self, src, dst, ssem, rsem):
        return pltpu.make_async_remote_copy(src_ref=src, dst_ref=dst, send_sem=ssem, recv_sem=rsem, device_id={'col': self.zc}, device_id_type=MESH)


def entry_barrier(pc):
    bar = pltpu.get_barrier_semaphore()
    for j in range(1, 8):
        pl.semaphore_signal(bar, inc=1, device_id={'row': (pc.r + j) % 8}, device_id_type=MESH)
    pl.semaphore_signal(bar, inc=1, device_id={'col': pc.zc}, device_id_type=MESH)
    pl.semaphore_wait(bar, 8)


class Gather:
    def __init__(self, pc, unit, part, ssem, rsem):
        self.pc, self.unit, self.part, self.ssem, self.rsem = pc, unit, part, ssem, rsem
        self.sent = []

    def _send(self, k, ref, row):
        cp = self.pc.to_row(ref, ref, self.ssem.at[k], self.rsem.at[k], row)
        cp.start()
        self.sent.append(cp)

    def _recv(self, k, ref):
        self.pc.to_row(ref, ref, self.ssem.at[k], self.rsem.at[k], self.pc.mate).wait_recv()

    def start(self):
        pc = self.pc
        own = self.unit(pc.r)
        self._send(0, own, pc.xn)
        self._send(1, own, pc.yn)
        self._send(2, own, pc.mate)

    def wait_mate(self):
        self._recv(2, self.unit(self.pc.mate))

    def relay(self):
        pc = self.pc
        self._recv(0, self.unit(pc.xn))
        self._send(3, self.part(pc.xn, 0), pc.yn)
        self._send(5, self.unit(pc.xn), pc.mate)
        self._recv(1, self.unit(pc.yn))
        self._send(4, self.part(pc.yn, 1), pc.xn)
        self._send(6, self.unit(pc.yn), pc.mate)

    def wait_mates(self):
        pc = self.pc
        self._recv(5, self.unit(pc.mate_x))
        self._recv(6, self.unit(pc.mate_y))

    def last(self):
        pc = self.pc
        self._recv(3, self.part(pc.dg, 0))
        self._recv(4, self.part(pc.dg, 1))
        self._send(7, self.unit(pc.dg), pc.mate)

    def finish(self):
        self._recv(7, self.unit(self.pc.mate_d))
        for cp in self.sent:
            cp.wait_send()
        self.sent = []


def whole_gather(pc, ref, ssem, rsem):
    half = ref.shape[1] // 2
    return Gather(pc, lambda q: ref.at[q], lambda q, h: ref.at[q, h * half:(h + 1) * half], ssem, rsem)


def lane_gather(pc, ref, lanes, ssem, rsem):
    half = ref.shape[1] // 2
    return Gather(pc, lambda q: ref.at[q, :, 0:lanes], lambda q, h: ref.at[q, h * half:(h + 1) * half, 0:lanes], ssem, rsem)


class Scatter:
    def __init__(self, pc, pi, rd, rx, ry, rz, ssem, rsem):
        self.pc, self.pi = pc, pi
        self.rd, self.rx, self.ry, self.rz = rd, rx, ry, rz
        self.ssem, self.rsem = ssem, rsem
        self.mates = (pc.mate_d, pc.mate_x, pc.mate_y, pc.mate)
        self.owns = (pc.dg, pc.xn, pc.yn, pc.r)
        hops = [(pi.at[q], rd.at[k], pc.mate) for k, q in enumerate(self.mates)]
        hops += [(pi.at[pc.dg, LO], rx.at[1], pc.xn), (pi.at[pc.dg, HI], ry.at[1], pc.yn)]
        hops += [(pi.at[pc.xn, LO], rx.at[0], pc.xn), (pi.at[pc.yn, HI], ry.at[0], pc.yn)]
        hops += [(pi.at[pc.yn, LO], rz.at[0], pc.yn), (pi.at[pc.xn, HI], rz.at[1], pc.xn)]
        self.hops = [pc.to_row(src, dst, ssem.at[k], rsem.at[k], to) for k, (src, dst, to) in enumerate(hops)]
        self.far = self.hops[4:6]
        self.near = self.hops[6:8]
        self.late = self.hops[8:]

    def item(self, a, xu, send_far=True, send_near=True, between=None):
        pc, pi = self.pc, self.pi
        x = jnp.concatenate([xu[0], xu[1]], axis=1)
        blocks = [slice(n, n + USERS) for n in range(0, SHARD, USERS)]

        def mates(j, _):
            q = choose(j, self.mates)
            for n in blocks:
                pi[q, :, n] = jnp.dot(x, a[q, :, n], preferred_element_type=F32)
            pc.to_row(pi.at[q], self.rd.at[j], self.ssem.at[j], self.rsem.at[j], pc.mate).start()
            return 0

        def owns(j, _):
            q = choose(j, self.owns)
            pc.to_row(pi.at[q], self.rd.at[j], self.ssem.at[j], self.rsem.at[j], pc.mate).wait_recv()
            for n in blocks:
                pi[q, :, n] = self.rd[j, :, n] + jnp.dot(x, a[q, :, n], preferred_element_type=F32)
            if send_far:
                @pl.when(j == 0)
                def _():
                    self.start_far()
            return 0

        lax.fori_loop(0, len(self.mates), mates, 0)
        if between is not None:
            between()
        lax.fori_loop(0, len(self.owns), owns, 0)
        if send_near:
            self.start_near()

    def start_far(self):
        for hop in self.far:
            hop.start()

    def start_near(self):
        for hop in self.near:
            hop.start()

    def second(self):
        pc, pi = self.pc, self.pi
        self.far[0].wait_recv()
        pi[pc.yn, LO] += self.rx[1]
        self.late[0].start()
        self.far[1].wait_recv()
        pi[pc.xn, HI] += self.ry[1]
        self.late[1].start()

    def result(self, emit):
        pc, pi = self.pc, self.pi
        self.near[0].wait_recv()
        self.near[1].wait_recv()
        self.late[0].wait_recv()
        emit(LO, pi[pc.r, LO] + self.rx[0] + self.rz[0])
        self.late[1].wait_recv()
        emit(HI, pi[pc.r, HI] + self.ry[0] + self.rz[1])
        for hop in self.hops:
            hop.wait_send()


def user_part(a, xi, up, shards, first=False):
    if first:
        up[...] = jnp.zeros_like(up)

    def body(j, _):
        q = choose(j, shards)
        for h in range(2):
            up[h] += lax.dot_general(xi[q], a[q, h * USERS:(h + 1) * USERS, :], NT, preferred_element_type=F32)
        return 0

    lax.fori_loop(0, len(shards), body, 0)


def user_half(a, xi, up, shards, h):
    def body(j, _):
        q = choose(j, shards)
        up[h] += lax.dot_general(xi[q], a[q, window(h, USERS), :], NT, preferred_element_type=F32)
        return 0

    lax.fori_loop(0, len(shards), body, 0)


def propagate(pc, a, xis, xus, ups, urs, scat, gath, zs, zr, fin_u, fin_i, gather_first=False, after_u3=None):
    me = pc
    sp, sq = scat
    gp, gq = gath
    near = (me.r, me.mate, me.xn, me.yn)
    far = (me.mate_x, me.mate_y, me.dg, me.mate_d)

    def users_and_send(ch, shards):
        up = ups[ch]
        user_half(a, xis[ch], up, shards, me.zc)
        cp = me.to_z(up.at[me.zc], urs[ch], zs.at[ch, 0], zr.at[ch, 0])
        cp.start()
        user_half(a, xis[ch], up, shards, me.c)
        return cp

    def z_sum(ch, cp):
        cp.wait()
        return ups[ch][me.c] + urs[ch][...]

    def z_share(ch, xu):
        cp = me.to_z(xu.at[me.c], xu.at[me.c], zs.at[ch, 1], zr.at[ch, 1])
        cp.start()
        return cp

    sq.item(a, xus[0], between=gp.relay if gather_first else None)
    if gather_first:
        gp.wait_mate()
    user_part(a, xis[0], ups[0], near, True)
    if gather_first:
        gp.last()
        gp.wait_mates()
        gp.finish()
    sq.second()
    cp = users_and_send(0, far)
    xus[1][me.c] = fin_u(1, z_sum(0, cp))
    share = z_share(0, xus[1])

    def keep1(rows, value):
        xis[1][me.r, rows] = fin_i(1, rows, value)

    sq.result(keep1)
    gq.start()
    share.wait()
    sp.item(a, xus[1], send_far=False, send_near=False)
    gq.relay()
    sp.start_far()
    sp.start_near()
    gq.wait_mate()
    user_part(a, xis[1], ups[1], near, True)
    gq.last()
    gq.wait_mates()
    user_part(a, xis[1], ups[1], far[:2])
    gq.finish()
    cp = users_and_send(1, far[2:])
    sp.second()
    xus[2][me.c] = fin_u(2, z_sum(1, cp))
    z_share(1, xus[2]).wait()
    sq.item(a, xus[2], send_near=False)

    def keep2(rows, value):
        xis[0][me.r, rows] = fin_i(2, rows, value)

    sp.result(keep2)
    gp.start()
    sq.start_near()
    user_part(a, xis[0], ups[0], near[:1], True)
    gp.relay()
    sq.second()
    gp.wait_mate()
    user_part(a, xis[0], ups[0], near[1:])
    gp.last()
    gp.wait_mates()
    user_part(a, xis[0], ups[0], far[:2])
    gp.finish()
    cp = users_and_send(0, far[2:])
    fin_u(3, z_sum(0, cp))
    if after_u3 is not None:
        after_u3()

    def keep3(rows, value):
        fin_i(3, rows, value)

    sq.result(keep3)


def comm_scratch():
    dma = pltpu.SemaphoreType.DMA
    return [
        pltpu.VMEM((ROWS, 2 * USERS, SHARD), BF16),
        pltpu.VMEM((TWO, ROWS, D, SHARD), BF16),
        pltpu.VMEM((THREE, TWO, D, USERS), BF16),
        pltpu.VMEM((TWO, TWO, D, USERS), F32),
        pltpu.VMEM((TWO, D, USERS), F32),
        pltpu.VMEM((TWO, ROWS, D, SHARD), F32),
        pltpu.VMEM((TWO, 4, D, SHARD), F32),
        pltpu.VMEM((TWO, 6, HALF, SHARD), F32),
        dma((6, ROWS)), dma((6, ROWS)), dma((TWO, 10)), dma((TWO, 10)), dma((TWO, 4)), dma((TWO, 4)),
    ]


def comm_objects(pc, a, xi, xu, up, ur, pi, rd, rxyz, gs, gr, ss, sr, zs, zr):
    scat = [Scatter(pc, pi.at[k], rd.at[k], rxyz.at[k, 0:2], rxyz.at[k, 2:4], rxyz.at[k, 4:6], ss.at[k], sr.at[k]) for k in range(2)]
    gath = [whole_gather(pc, xi.at[k], gs.at[k], gr.at[k]) for k in range(2)]
    return dict(pc=pc, a=a, xis=[xi.at[0], xi.at[1]], xus=[xu.at[k] for k in range(3)], ups=[up.at[0], up.at[1]],
                urs=[ur.at[0], ur.at[1]], scat=scat, gath=gath, zs=zs, zr=zr)


def one_hot(ids, rows):
    shape = (rows, ids.shape[1])
    wide = jnp.broadcast_to(ids.astype(jnp.int16), shape)
    return jnp.where(wide == lax.broadcasted_iota(jnp.int16, shape, 0), jnp.ones((), BF16), jnp.zeros((), BF16))


def split3(v):
    v1 = v.astype(BF16)
    rest = v - v1.astype(F32)
    v2 = rest.astype(BF16)
    v3 = (rest - v2.astype(F32)).astype(BF16)
    return jnp.concatenate([v1, v2, v3], axis=0)


def mega_kernel(m_hbm, u0, i0, ids, eu, ei, loss, gu, gi, *scratch):
    comm, rest = scratch[:14], scratch[14:]
    stage, rowacc, colacc, dpi, drecv, sib, du, dur, su, accu, acci, eall, egat, cg, msem, ds, dr = rest
    pc = Place()
    objs = comm_objects(pc, *comm)
    a, xi, xu, up, ur, pi = comm[:6]
    gs, gr = comm[8:10]
    zs, zr = comm[12:]
    xi0, xi1 = xi.at[0], xi.at[1]

    def z_share(ref, ch, k):
        cp = pc.to_z(ref, ref, zs.at[ch, k], zr.at[ch, k])
        cp.start()
        return cp

    per_shard = 2 * USERS // GROUP

    def fetch(k):
        block = m_hbm.at[window(k % per_shard, GROUP), window(k // per_shard, SHARD)]
        return pltpu.make_async_copy(block, stage.at[k % SLOTS], msem.at[k % SLOTS])

    for k in range(SLOTS):
        fetch(k).start()
    xi0[pc.r] = i0[...]
    xu[0, pc.c] = u0[...]
    accu[...] = u0[...].astype(F32)
    acci[...] = i0[...].astype(F32)
    rowacc[...] = jnp.zeros_like(rowacc)
    entry_barrier(pc)
    gp, gq = objs['gath']
    gp.start()
    share0 = z_share(xu.at[0, pc.c], 0, 1)
    strip = 2 * ROWS

    def degree_copy(j, q):
        return pc.to_row(dpi.at[q], drecv.at[j - 1, q], ds.at[j - 1], dr.at[j - 1], (pc.r + j) % ROWS)

    def shard(q, _):
        colacc[...] = jnp.zeros_like(colacc)

        def block(t, _):
            k = q * per_shard + t
            slot = k % SLOTS
            fetch(k).wait()

            def rows16(g, cols):
                here = window(g, strip)
                there = pl.ds(pl.multiple_of(t * GROUP + g * strip, strip), strip)
                racc = rowacc[there, :]
                out = []
                for n in range(0, SHARD, GROUP):
                    m = stage[slot, here, n:n + GROUP]
                    a[q, there, n:n + GROUP] = m.astype(F32).astype(BF16)
                    out.append(cols[n // GROUP] + (m[:ROWS] + m[ROWS:]))
                    racc = racc + m
                rowacc[there, :] = racc
                return tuple(out)

            lanes = range(0, SHARD, GROUP)
            cols = lax.fori_loop(0, GROUP // strip, rows16, tuple(colacc[:, n:n + GROUP] for n in lanes))
            for n, col in zip(lanes, cols):
                colacc[:, n:n + GROUP] = col

            @pl.when(k + SLOTS < ROWS * per_shard)
            def _():
                fetch(k + SLOTS).start()

            return 0

        lax.fori_loop(0, per_shard, block, 0)
        sums = jnp.sum(colacc[...], axis=0, keepdims=True)
        for s in range(ROWS):
            dpi[q, s:s + 1, :] = sums[:, s * FOLD:(s + 1) * FOLD]
        for j in range(1, ROWS):
            degree_copy(j, q).start()
        return 0

    lax.fori_loop(0, 3, shard, 0)
    gp.relay()
    lax.fori_loop(3, 5, shard, 0)
    gp.last()
    gp.wait_mate()
    gp.wait_mates()
    lax.fori_loop(5, ROWS, shard, 0)
    sums = jnp.sum(rowacc[...].astype(F32).T, axis=0, keepdims=True)
    du[...] = jnp.broadcast_to(sums, du.shape).astype(jnp.int32)
    zc = pc.to_z(du, dur, ds.at[ROWS - 1], dr.at[ROWS - 1])
    zc.start()
    gp.finish()
    share0.wait()
    zc.wait()
    scale = lax.rsqrt(jnp.maximum(du[...] + dur[...], 1).astype(F32))
    su[...] = jnp.broadcast_to(scale[:1], (GROUP, 2 * USERS)).T
    for j in range(1, ROWS):
        whole = pc.to_row(dpi, drecv.at[j - 1], ds.at[j - 1], dr.at[j - 1], (pc.r + j) % ROWS)
        whole.wait()

    def form(q, _):
        deg = dpi[q]
        for j in range(ROWS - 1):
            deg = deg + drecv[j, q]
        scale = lax.rsqrt(jnp.maximum(deg, 1).astype(F32))
        for s in range(ROWS):
            sib[:, s * FOLD:(s + 1) * FOLD] = jnp.broadcast_to(scale[s:s + 1], (ROWS, FOLD))
        tall = 4 * ROWS

        def rows32(t, _):
            rows = window(t, tall)
            sub = su[rows, :]
            for n in range(0, SHARD, GROUP):
                col = sib[:, n:n + GROUP]
                both = (sub * jnp.concatenate([col, col, col, col], axis=0)).astype(BF16)
                a[q, rows, n:n + GROUP] = a[q, rows, n:n + GROUP] * both
            return 0

        lax.fori_loop(0, 2 * USERS // tall, rows32, 0)
        return 0

    lax.fori_loop(0, ROWS, form, 0)

    def fin_u(k, total):
        nxt = total.astype(BF16)
        accu[...] += nxt.astype(F32)
        return nxt

    def fin_i(k, rows, total):
        nxt = total.astype(BF16)
        acci[rows] += nxt.astype(F32)
        return nxt

    lane_c, row_c = window(pc.c, USERS), window(pc.c, D)
    chunk = pc.r * 2 + pc.c
    role = BATCH // USERS
    pending = []
    gu_all = whole_gather(pc, eall, gs.at[2], gr.at[2])
    ge = whole_gather(pc, egat, gs.at[3], gr.at[3])

    def after_u3():
        e = (accu[...] / (LAYERS + 1)).astype(BF16)
        eu[...] = e
        eall[pc.r, row_c, :] = e
        share = z_share(eall.at[pc.r, row_c, :], 0, 1)
        share.wait()
        gu_all.start()

    propagate(fin_u=fin_u, fin_i=fin_i, after_u3=after_u3, **objs)

    e = (acci[...] / (LAYERS + 1)).astype(BF16)
    ei[...] = e
    xi1[pc.r] = e
    gq.start()

    up[0] = jnp.zeros_like(up[0])

    def diffs(shards):
        def body(j, _):
            q = choose(j, shards)
            base = pc.c * ITEMS + q * SHARD
            for h in range(2):
                pos = ids[pl.ds(role + pc.r * 2 + h, 1), :] - base
                neg = ids[pl.ds(2 * role + pc.r * 2 + h, 1), :] - base
                acc = up[0, h]
                for s in range(0, SHARD, FOLD):
                    pick = one_hot(pos - s, FOLD) - one_hot(neg - s, FOLD)
                    acc = acc + jnp.dot(xi1[q, :, s:s + FOLD], pick, preferred_element_type=F32)
                up[0, h] = acc
            return 0

        lax.fori_loop(0, len(shards), body, 0)

    def users(q, acc):
        for h in range(2):
            pick = one_hot(ids[pl.ds(chunk, 1), :] - (q * 2 + h) * USERS, USERS)
            acc = acc + jnp.dot(eall[q, h * D:(h + 1) * D, :], pick, preferred_element_type=F32)
        return acc

    gu_all.relay()
    gu_all.last()
    diffs((pc.r,))
    gq.relay()
    gu_all.wait_mate()
    gu_all.wait_mates()
    gu_all.finish()
    e_user = lax.fori_loop(0, ROWS, users, jnp.zeros((D, USERS), F32))
    egat[pc.r, row_c, :] = e_user.astype(BF16)
    z1 = z_share(egat.at[pc.r, row_c, :], 1, 1)
    gq.wait_mate()
    gq.last()
    diffs((pc.mate, pc.xn, pc.yn))
    z1.wait()
    ge.start()
    gq.wait_mates()
    gq.finish()
    diffs((pc.mate_x, pc.mate_y, pc.dg, pc.mate_d))
    part = pc.to_z(up.at[0, pc.zc], ur.at[0], zs.at[0, 0], zr.at[0, 0])
    part.start()
    ge.relay()
    ge.last()
    part.wait()
    d = up[0, pc.c] + ur[0]
    margin = jnp.sum(e_user * d, axis=0, keepdims=True)
    soft = jnp.maximum(-margin, 0.0) + jnp.log1p(jnp.exp(-jnp.abs(margin)))
    coef = -jax.nn.sigmoid(-margin) / BATCH
    row8 = window(pc.c, ROWS)
    wide = (ROWS // 2, USERS)
    cg[pc.r, row8, :] = jnp.concatenate([jnp.broadcast_to(coef, wide), jnp.broadcast_to(soft, wide)], axis=0)
    z3 = z_share(cg.at[pc.r, row8, :], 1, 3)
    pi[0, pc.r, :, lane_c] = coef * d
    z2 = z_share(pi.at[0, pc.r, :, lane_c], 1, 2)
    gv = lane_gather(pc, pi.at[0], 2 * USERS, gs.at[4], gr.at[4])
    gc = whole_gather(pc, cg, gs.at[5], gr.at[5])
    z3.wait()
    gc.start()
    z2.wait()
    gv.start()
    acc = pi.at[1]
    acc[:6] = jnp.zeros((6, D, SHARD), F32)
    ge.wait_mate()
    ge.wait_mates()
    ge.finish()
    gc.relay()
    gc.last()
    gc.wait_mate()
    gc.wait_mates()
    gc.finish()
    item_base = pc.c * ITEMS + pc.r * SHARD

    def item_grads(q, total):
        for h in range(2):
            k = q * 2 + h
            co = cg[q, h * ROWS:h * ROWS + 1, :]
            total = total + cg[q, h * ROWS + 4:h * ROWS + 5, :]
            v = split3(co * egat[q, h * D:(h + 1) * D, :].astype(F32))
            pos = ids[pl.ds(role + k, 1), :] - item_base
            neg = ids[pl.ds(2 * role + k, 1), :] - item_base
            for n in range(0, SHARD, USERS):
                picks = [one_hot(pos - b, FOLD) - one_hot(neg - b, FOLD) for b in (n, n + FOLD)]
                part_g = lax.dot_general(v, jnp.concatenate(picks, axis=0), NT, preferred_element_type=F32)
                for j in range(3):
                    acc[j, :, n:n + USERS] += part_g[j * D:(j + 1) * D]
        return total

    def user_grads(q, _):
        for h in range(2):
            w = split3(pi[0, q, :, h * USERS:(h + 1) * USERS])
            pick = one_hot(ids[pl.ds(q * 2 + h, 1), :] - chunk * USERS, USERS)
            part_g = lax.dot_general(w, pick, NT, preferred_element_type=F32)
            for j in range(3):
                acc[3 + j, :, :USERS] += part_g[j * D:(j + 1) * D]
        return 0

    total = lax.fori_loop(0, 4, item_grads, jnp.zeros((1, USERS), F32))
    gv.relay()
    total = lax.fori_loop(4, ROWS, item_grads, total)
    gv.last()
    loss[...] = jnp.broadcast_to(jnp.sum(total, axis=1, keepdims=True) / BATCH, loss.shape)
    src_i, src_u = acci, accu
    src_i[...] = ((acc[0] + acc[1]) + acc[2]) / (LAYERS + 1)
    gv.wait_mate()
    gv.wait_mates()
    gv.finish()

    objs['xis'], objs['gath'] = objs['xis'][::-1], objs['gath'][::-1]
    gp, gq = objs['gath']
    xi1[pc.r] = src_i[...].astype(BF16)
    gp.start()
    lax.fori_loop(0, ROWS, user_grads, 0)
    src_u[...] = ((acc[3, :, :USERS] + acc[4, :, :USERS]) + acc[5, :, :USERS]) / (LAYERS + 1)
    xu[0, pc.c] = src_u[...].astype(BF16)
    z_share(xu.at[0, pc.c], 0, 1).wait()

    def back_u(k, total):
        value = src_u[...] + total
        if k == LAYERS:
            gu[...] = value
        return value.astype(BF16)

    def back_i(k, rows, total):
        value = src_i[rows] + total
        if k == LAYERS:
            gi[rows] = value
        return value.astype(BF16)

    propagate(fin_u=back_u, fin_i=back_i, gather_first=True, **objs)


def mega_call(mask_blk, u0, i0, ids):
    dma = pltpu.SemaphoreType.DMA
    vm = pl.BlockSpec(memory_space=pltpu.VMEM)
    hbm = pl.BlockSpec(memory_space=pl.ANY)
    i32 = jnp.int32
    shape = jax.ShapeDtypeStruct
    return pl.pallas_call(
        mega_kernel,
        name='mega',
        out_shape=(shape((D, USERS), BF16), shape((D, SHARD), BF16), shape((ROWS, GROUP), F32), shape((D, USERS), F32), shape((D, SHARD), F32)),
        in_specs=[hbm, vm, vm, vm],
        out_specs=(vm, vm, vm, vm, vm),
        scratch_shapes=comm_scratch() + [
            pltpu.VMEM((SLOTS, GROUP, SHARD), i32),
            pltpu.VMEM((2 * USERS, GROUP), i32),
            pltpu.VMEM((ROWS, SHARD), i32),
            pltpu.VMEM((ROWS, ROWS, FOLD), i32),
            pltpu.VMEM((ROWS - 1, ROWS, ROWS, FOLD), i32),
            pltpu.VMEM((ROWS, SHARD), F32),
            pltpu.VMEM((ROWS, 2 * USERS), i32),
            pltpu.VMEM((ROWS, 2 * USERS), i32),
            pltpu.VMEM((2 * USERS, GROUP), F32),
            pltpu.VMEM((D, USERS), F32),
            pltpu.VMEM((D, SHARD), F32),
            pltpu.VMEM((ROWS, 2 * D, USERS), BF16),
            pltpu.VMEM((ROWS, 2 * D, USERS), BF16),
            pltpu.VMEM((ROWS, 2 * ROWS, USERS), F32),
            dma((SLOTS,)), dma((ROWS,)), dma((ROWS,)),
        ],
        compiler_params=pltpu.CompilerParams(collective_id=0, has_side_effects=True, vmem_limit_bytes=VMEM_LIMIT),
    )(mask_blk, u0, i0, ids)


def solution(mesh):
    def local_fn(mask_blk, user_emb, item_emb, triples):
        ids = triples.T.reshape(3 * BATCH // USERS, USERS)
        eu, ei, loss, gu, gi = mega_call(mask_blk, user_emb.T, item_emb.T, ids)
        return eu.T, ei.T, loss[0, 0], gu.T, gi.T

    user_spec = P(('row', 'col'), None)
    item_spec = P(('col', 'row'), None)
    return jax.shard_map(local_fn, mesh=mesh, in_specs=(P('row', 'col'), user_spec, item_spec, P()), out_specs=(user_spec, item_spec, P(), user_spec, item_spec), check_vma=False)
```

```python
import functools

import jax
import jax.numpy as jnp
from jax import lax
from jax.experimental import pallas as pl
from jax.experimental.pallas import tpu as pltpu
from jax.sharding import PartitionSpec as P

LAYERS = 3
MESH = pl.DeviceIdType.MESH
F32 = jnp.float32
BF16 = jnp.bfloat16
VMEM_LIMIT = 67_043_328
NT = (((1,), (1,)), ((), ()))
NONE, ONE, TWO, THREE = range(4)
D = 64
HALF = D // 2
SHARD = 2048
USERS = 512
GROUP = 128
FOLD = 256
ROWS = 8
SLOTS = 12
BATCH = 8192
ITEMS = ROWS * SHARD
LO, HI = slice(0, HALF), slice(HALF, D)


def choose(j, values):
    out = values[-1]
    for k in range(len(values) - 1):
        out = jnp.where(j == k, values[k], out)
    return out


def window(k, size):
    return pl.ds(pl.multiple_of(k * size, size), size)


class Place:
    def __init__(self):
        r = lax.axis_index('row')
        c = lax.axis_index('col')
        core = r % 2
        x = (r // 2) % 2
        y = r // 4
        self.r, self.c, self.core = r, c, core
        self.mate = r + 1 - 2 * core
        self.xn = r + 2 - 4 * x
        self.yn = r + 4 - 8 * y
        self.dg = self.xn + 4 - 8 * y
        self.zc = 1 - c
        d = 1 - 2 * core
        self.mate_x, self.mate_y, self.mate_d = self.xn + d, self.yn + d, self.dg + d

    def to_row(self, src, dst, ssem, rsem, row):
        return pltpu.make_async_remote_copy(src_ref=src, dst_ref=dst, send_sem=ssem, recv_sem=rsem, device_id={'row': row}, device_id_type=MESH)

    def to_z(self, src, dst, ssem, rsem):
        return pltpu.make_async_remote_copy(src_ref=src, dst_ref=dst, send_sem=ssem, recv_sem=rsem, device_id={'col': self.zc}, device_id_type=MESH)


def entry_barrier(pc):
    bar = pltpu.get_barrier_semaphore()
    for j in range(1, 8):
        pl.semaphore_signal(bar, inc=1, device_id={'row': (pc.r + j) % 8}, device_id_type=MESH)
    pl.semaphore_signal(bar, inc=1, device_id={'col': pc.zc}, device_id_type=MESH)
    pl.semaphore_wait(bar, 8)


class Gather:
    def __init__(self, pc, unit, part, ssem, rsem):
        self.pc, self.unit, self.part = pc, unit, part
        self.ssem, self.rsem = ssem, rsem
        own = unit(pc.r)
        hops = [(own, pc.xn), (own, pc.yn), (own, pc.mate), (part(pc.xn, 0), pc.yn), (part(pc.yn, 1), pc.xn)]
        hops += [(unit(pc.xn), pc.mate), (unit(pc.yn), pc.mate), (unit(pc.dg), pc.mate)]
        self.hops = [pc.to_row(ref, ref, ssem.at[k], rsem.at[k], to) for k, (ref, to) in enumerate(hops)]

    def _recv(self, k, ref):
        self.pc.to_row(ref, ref, self.ssem.at[k], self.rsem.at[k], self.pc.mate).wait_recv()

    def start(self):
        for hop in self.hops[:3]:
            hop.start()

    def wait_mate(self):
        self._recv(2, self.unit(self.pc.mate))

    def relay(self):
        pc, hops = self.pc, self.hops
        self._recv(0, self.unit(pc.xn))
        hops[3].start()
        hops[5].start()
        self._recv(1, self.unit(pc.yn))
        hops[4].start()
        hops[6].start()

    def wait_mates(self):
        pc = self.pc
        self._recv(5, self.unit(pc.mate_x))
        self._recv(6, self.unit(pc.mate_y))

    def last(self):
        pc = self.pc
        self._recv(3, self.part(pc.dg, 0))
        self._recv(4, self.part(pc.dg, 1))
        self.hops[7].start()

    def finish(self):
        self._recv(7, self.unit(self.pc.mate_d))
        for hop in self.hops:
            hop.wait_send()


def whole_gather(pc, ref, ssem, rsem):
    half = ref.shape[1] // 2
    return Gather(pc, lambda q: ref.at[q], lambda q, h: ref.at[q, h * half:(h + 1) * half], ssem, rsem)


class Scatter:
    def __init__(self, pc, pi, rd, rx, ry, rz, ssem, rsem):
        self.pc, self.pi = pc, pi
        self.rd, self.rx, self.ry, self.rz = rd, rx, ry, rz
        self.ssem, self.rsem = ssem, rsem
        self.mates = (pc.mate_d, pc.mate_x, pc.mate_y, pc.mate)
        self.owns = (pc.dg, pc.xn, pc.yn, pc.r)
        hops = [(pi.at[q], rd.at[k], pc.mate) for k, q in enumerate(self.mates)]
        hops += [(pi.at[pc.dg, LO], rx.at[1], pc.xn), (pi.at[pc.dg, HI], ry.at[1], pc.yn)]
        hops += [(pi.at[pc.xn, LO], rx.at[0], pc.xn), (pi.at[pc.yn, HI], ry.at[0], pc.yn)]
        hops += [(pi.at[pc.yn, LO], rz.at[0], pc.yn), (pi.at[pc.xn, HI], rz.at[1], pc.xn)]
        self.hops = [pc.to_row(src, dst, ssem.at[k], rsem.at[k], to) for k, (src, dst, to) in enumerate(hops)]
        self.far = self.hops[4:6]
        self.near = self.hops[6:8]
        self.late = self.hops[8:]

    def item(self, a, xu, send_far=True, send_near=True, between=None):
        pc, pi = self.pc, self.pi
        x = jnp.concatenate([xu[0], xu[1]], axis=1)
        blocks = [slice(n, n + USERS) for n in range(0, SHARD, USERS)]

        def for_mate(j):
            q = choose(j, self.mates)
            for n in blocks:
                pi[q, :, n] = jnp.dot(x, a[q, :, n], preferred_element_type=F32)
            pc.to_row(pi.at[q], self.rd.at[j], self.ssem.at[j], self.rsem.at[j], pc.mate).start()

        def for_self(j):
            q = choose(j, self.owns)
            pc.to_row(pi.at[q], self.rd.at[j], self.ssem.at[j], self.rsem.at[j], pc.mate).wait_recv()
            for n in blocks:
                pi[q, :, n] = self.rd[j, :, n] + jnp.dot(x, a[q, :, n], preferred_element_type=F32)

        def both(j, _):
            for_mate(j + 1)
            if between is not None:
                @pl.when(j == 1)
                def _():
                    between()
            for_self(j)
            if send_far:
                @pl.when(j == 0)
                def _():
                    self.start_far()
            if send_near:
                for k in range(2):
                    @pl.when(j == k + 1)
                    def _(k=k):
                        self.near[k].start()
            return 0

        for_mate(0)
        lax.fori_loop(0, 3, both, 0)
        for_self(3)

    def start_far(self):
        for hop in self.far:
            hop.start()

    def start_near(self):
        for hop in self.near:
            hop.start()

    def second(self):
        pc, pi = self.pc, self.pi
        self.far[0].wait_recv()
        pi[pc.yn, LO] += self.rx[1]
        self.late[0].start()
        self.far[1].wait_recv()
        pi[pc.xn, HI] += self.ry[1]
        self.late[1].start()

    def result(self, emit):
        pc, pi = self.pc, self.pi
        self.near[0].wait_recv()
        self.near[1].wait_recv()
        self.late[0].wait_recv()
        emit(LO, pi[pc.r, LO] + self.rx[0] + self.rz[0])
        self.late[1].wait_recv()
        emit(HI, pi[pc.r, HI] + self.ry[0] + self.rz[1])
        for hop in self.hops:
            hop.wait_send()


def user_part(a, xi, up, shards, first=False):
    if first:
        up[...] = jnp.zeros_like(up)

    def body(j, _):
        q = choose(j, shards)
        for h in range(2):
            up[h] += lax.dot_general(xi[q], a[q, h * USERS:(h + 1) * USERS, :], NT, preferred_element_type=F32)
        return 0

    lax.fori_loop(0, len(shards), body, 0)


def user_half(a, xi, up, shards, h):
    def body(j, _):
        q = choose(j, shards)
        up[h] += lax.dot_general(xi[q], a[q, window(h, USERS), :], NT, preferred_element_type=F32)
        return 0

    lax.fori_loop(0, len(shards), body, 0)


def propagate(pc, a, xis, xus, ups, urs, scat, gath, zs, zr, fin_u, fin_i, gather_first=False):
    me = pc
    sp, sq = scat
    gp, gq = gath
    near = (me.r, me.mate, me.xn, me.yn)
    far = (me.mate_x, me.mate_y, me.dg, me.mate_d)

    def swap(ch, h):
        return me.to_z(ups[ch].at[h], urs[ch].at[h], zs.at[ch, h], zr.at[ch, h])

    def send_users(ch, shards):
        def body(h, _):
            user_half(a, xis[ch], ups[ch], shards, h)
            swap(ch, h).start()
            return 0

        lax.fori_loop(0, 2, body, 0)

    def join_users(ch, k, xu):
        for h in range(2):
            swap(ch, h).wait()
            nxt = fin_u(k, h, ups[ch][h] + urs[ch][h])
            if xu is not None:
                xu[h] = nxt

    sq.item(a, xus[0], between=gp.relay if gather_first else None)
    if gather_first:
        gp.wait_mate()
    user_part(a, xis[0], ups[0], near, True)
    if gather_first:
        gp.last()
        gp.wait_mates()
        gp.finish()
    sq.second()
    send_users(0, far)

    def keep1(rows, value):
        xis[1][me.r, rows] = fin_i(1, rows, value)

    sq.result(keep1)
    gq.start()
    join_users(0, 1, xus[1])
    sp.item(a, xus[1], send_far=False, send_near=False)
    gq.relay()
    sp.start_far()
    sp.start_near()
    gq.wait_mate()
    user_part(a, xis[1], ups[1], near, True)
    gq.last()
    gq.wait_mates()
    user_part(a, xis[1], ups[1], far[:2])
    gq.finish()
    send_users(1, far[2:])
    sp.second()
    join_users(1, 2, xus[2])

    def keep2(rows, value):
        xis[0][me.r, rows] = fin_i(2, rows, value)

    def next_gather():
        sp.result(keep2)
        gp.start()

    sq.item(a, xus[2], send_near=False, between=next_gather)
    user_part(a, xis[0], ups[0], near[:1], True)
    gp.relay()
    sq.start_near()
    gp.wait_mate()
    user_part(a, xis[0], ups[0], near[1:])
    sq.second()
    gp.last()
    gp.wait_mates()
    user_part(a, xis[0], ups[0], far[:2])
    gp.finish()
    send_users(0, far[2:])
    join_users(0, 3, None)

    def keep3(rows, value):
        fin_i(3, rows, value)

    sq.result(keep3)


def comm_scratch():
    dma = pltpu.SemaphoreType.DMA
    return [
        pltpu.VMEM((ROWS, 2 * USERS, SHARD), BF16),
        pltpu.VMEM((TWO, ROWS, D, SHARD), BF16),
        pltpu.VMEM((THREE, TWO, D, USERS), BF16),
        pltpu.VMEM((TWO, TWO, D, USERS), F32),
        pltpu.VMEM((TWO, TWO, D, USERS), F32),
        pltpu.VMEM((TWO, 4, D, SHARD), F32),
        pltpu.VMEM((TWO, 6, HALF, SHARD), F32),
        dma((5, ROWS)), dma((5, ROWS)), dma((TWO, 10)), dma((TWO, 10)), dma((TWO, 4)), dma((TWO, 4)),
    ]


def comm_objects(pc, pi, a, xi, xu, up, ur, rd, rxyz, gs, gr, ss, sr, zs, zr):
    scat = [Scatter(pc, pi.at[k], rd.at[k], rxyz.at[k, 0:2], rxyz.at[k, 2:4], rxyz.at[k, 4:6], ss.at[k], sr.at[k]) for k in range(2)]
    gath = [whole_gather(pc, xi.at[k], gs.at[k], gr.at[k]) for k in range(2)]
    return dict(pc=pc, a=a, xis=[xi.at[0], xi.at[1]], xus=[xu.at[k] for k in range(3)], ups=[up.at[0], up.at[1]],
                urs=[ur.at[0], ur.at[1]], scat=scat, gath=gath, zs=zs, zr=zr)


def one_hot(ids, rows):
    shape = (rows, ids.shape[1])
    wide = jnp.broadcast_to(ids.astype(jnp.int16), shape)
    return jnp.where(wide == lax.broadcasted_iota(jnp.int16, shape, 0), jnp.ones((), BF16), jnp.zeros((), BF16))


def split3(v):
    v1 = v.astype(BF16)
    rest = v - v1.astype(F32)
    v2 = rest.astype(BF16)
    v3 = (rest - v2.astype(F32)).astype(BF16)
    return jnp.concatenate([v1, v2, v3], axis=0)


def mega_kernel(m_hbm, u0, i0, ids, eu, ei, loss, gu, gi, *scratch):
    comm, rest = scratch[:13], scratch[13:]
    pc = Place()
    i32 = jnp.int32

    def first(stage, rowacc, colacc, sib, su, msem):
        form_adjacency(pc, m_hbm, u0, i0, comm, rest, stage, rowacc, colacc, sib, su, msem)

    pl.run_scoped(
        first,
        pltpu.VMEM((SLOTS, GROUP, SHARD), i32), pltpu.VMEM((2 * USERS, GROUP), i32), pltpu.VMEM((ROWS, SHARD), i32),
        pltpu.VMEM((ROWS, SHARD), F32), pltpu.VMEM((2 * USERS, GROUP), F32), pltpu.SemaphoreType.DMA((SLOTS,)),
    )
    pl.run_scoped(lambda pi: chains(pc, pi, ids, eu, ei, loss, gu, gi, comm, rest), pltpu.VMEM((TWO, ROWS, D, SHARD), F32))


def z_share(pc, ref, ssem, rsem):
    cp = pc.to_z(ref, ref, ssem, rsem)
    cp.start()
    return cp


def form_adjacency(pc, m_hbm, u0, i0, comm, rest, stage, rowacc, colacc, sib, su, msem):
    dpi, drecv, du, dur, accu, acci = rest[:6]
    ds, dr = rest[-2:]
    a, xi, xu = comm[:3]
    zs, zr = comm[11:]
    xi0 = xi.at[0]
    gp = whole_gather(pc, xi0, comm[7].at[0], comm[8].at[0])

    per_shard = 2 * USERS // GROUP

    def fetch(k):
        block = m_hbm.at[window(k % per_shard, GROUP), window(k // per_shard, SHARD)]
        return pltpu.make_async_copy(block, stage.at[k % SLOTS], msem.at[k % SLOTS])

    for k in range(SLOTS):
        fetch(k).start()
    xi0[pc.r] = i0[...]
    xu[0, pc.c] = u0[...]
    acci[...] = i0[...].astype(F32)
    rowacc[...] = jnp.zeros_like(rowacc)
    entry_barrier(pc)
    gp.start()
    share0 = z_share(pc, xu.at[0, pc.c], zs.at[0, 3], zr.at[0, 3])
    strip = 2 * ROWS

    def degree_copy(j, q):
        return pc.to_row(dpi.at[q], drecv.at[j - 1, q], ds.at[j - 1], dr.at[j - 1], (pc.r + j) % ROWS)

    def shard(q, _):
        colacc[...] = jnp.zeros_like(colacc)

        def block(t, _):
            k = q * per_shard + t
            slot = k % SLOTS
            fetch(k).wait()

            def rows16(g, cols):
                here = window(g, strip)
                there = pl.ds(pl.multiple_of(t * GROUP + g * strip, strip), strip)
                racc = rowacc[there, :]
                out = []
                for n in range(0, SHARD, GROUP):
                    m = stage[slot, here, n:n + GROUP]
                    a[q, there, n:n + GROUP] = m.astype(F32).astype(BF16)
                    out.append(cols[n // GROUP] + (m[:ROWS] + m[ROWS:]))
                    racc = racc + m
                rowacc[there, :] = racc
                return tuple(out)

            lanes = range(0, SHARD, GROUP)
            cols = lax.fori_loop(0, GROUP // strip, rows16, tuple(colacc[:, n:n + GROUP] for n in lanes))
            for n, col in zip(lanes, cols):
                colacc[:, n:n + GROUP] = col

            @pl.when(k + SLOTS < ROWS * per_shard)
            def _():
                fetch(k + SLOTS).start()

            return 0

        lax.fori_loop(0, per_shard, block, 0)
        sums = jnp.sum(colacc[...], axis=0, keepdims=True)
        for s in range(ROWS):
            dpi[q, s:s + 1, :] = sums[:, s * FOLD:(s + 1) * FOLD]
        for j in range(1, ROWS):
            degree_copy(j, q).start()
        return 0

    lax.fori_loop(0, 3, shard, 0)
    gp.relay()
    lax.fori_loop(3, 5, shard, 0)
    gp.last()
    gp.wait_mate()
    gp.wait_mates()
    lax.fori_loop(5, ROWS, shard, 0)
    sums = jnp.sum(rowacc[...].astype(F32).T, axis=0, keepdims=True)
    du[...] = jnp.broadcast_to(sums, du.shape).astype(jnp.int32)
    zc = pc.to_z(du, dur, ds.at[ROWS - 1], dr.at[ROWS - 1])
    zc.start()
    gp.finish()
    share0.wait()
    accu[...] = xu[0].astype(F32)
    zc.wait()
    scale = lax.rsqrt(jnp.maximum(du[...] + dur[...], 1).astype(F32))
    su[...] = jnp.broadcast_to(scale[:1], (GROUP, 2 * USERS)).T
    for j in range(1, ROWS):
        whole = pc.to_row(dpi, drecv.at[j - 1], ds.at[j - 1], dr.at[j - 1], (pc.r + j) % ROWS)
        whole.wait()

    def form(q, _):
        deg = dpi[q]
        for j in range(ROWS - 1):
            deg = deg + drecv[j, q]
        scale = lax.rsqrt(jnp.maximum(deg, 1).astype(F32))
        for s in range(ROWS):
            sib[:, s * FOLD:(s + 1) * FOLD] = jnp.broadcast_to(scale[s:s + 1], (ROWS, FOLD))
        tall = ROWS * ROWS

        def rows64(t, _):
            rows = window(t, tall)
            sub = su[rows, :]
            for n in range(0, SHARD, GROUP):
                col = sib[:, n:n + GROUP]
                both = (sub * jnp.concatenate([col] * ROWS, axis=0)).astype(BF16)
                a[q, rows, n:n + GROUP] = a[q, rows, n:n + GROUP] * both
            return 0

        lax.fori_loop(0, 2 * USERS // tall, rows64, 0)
        return 0

    lax.fori_loop(0, ROWS, form, 0)


def pack_rows(x):
    return jnp.concatenate([row[:, n:n + GROUP] for row in x for n in range(0, USERS, GROUP)], axis=0)


def unpack_row(tile, h):
    rows = USERS // GROUP
    return jnp.concatenate([tile[k:k + 1] for k in range(h * rows, (h + 1) * rows)], axis=1)


def chains(pc, pi, ids, eu, ei, loss, gu, gi, comm, rest):
    _, _, _, _, accu, acci, eall, egat, cg, mg, ds, dr = rest
    objs = comm_objects(pc, pi, *comm)
    a, xi, xu, up, ur, rd = comm[:6]
    gs, gr = comm[7:9]
    zs, zr = comm[11:]
    xi1 = xi.at[1]
    gp, gq = objs['gath']

    def fin_u(k, h, total):
        nxt = total.astype(BF16)
        accu[h] += nxt.astype(F32)
        return nxt

    def fin_i(k, rows, total):
        nxt = total.astype(BF16)
        acci[rows] += nxt.astype(F32)
        return nxt

    role = BATCH // USERS
    gu_all = whole_gather(pc, eall, gs.at[2], gr.at[2])
    ge = whole_gather(pc, egat, gs.at[3], gr.at[3])
    propagate(fin_u=fin_u, fin_i=fin_i, **objs)

    e = (acci[...] / (LAYERS + 1)).astype(BF16)
    xi1[pc.r] = e
    gq.start()
    ei[...] = e
    for h in range(2):
        eall[pc.r, h * D:(h + 1) * D, :] = (accu[h] / (LAYERS + 1)).astype(BF16)
    gu_all.start()
    eu[...] = (accu[pc.c] / (LAYERS + 1)).astype(BF16)

    dif, eus = up.at[0], up.at[1]
    dif[...] = jnp.zeros_like(dif)
    eus[...] = jnp.zeros_like(eus)

    def diffs(shards):
        def body(j, _):
            q = choose(j, shards)
            base = pc.c * ITEMS + q * SHARD
            for h in range(2):
                pos = ids[pl.ds(role + pc.r * 2 + h, 1), :] - base
                neg = ids[pl.ds(2 * role + pc.r * 2 + h, 1), :] - base
                acc = dif[h]
                for s in range(0, SHARD, FOLD):
                    pick = one_hot(pos - s, FOLD) - one_hot(neg - s, FOLD)
                    acc = acc + jnp.dot(xi1[q, :, s:s + FOLD], pick, preferred_element_type=F32)
                dif[h] = acc
            return 0

        lax.fori_loop(0, len(shards), body, 0)

    def users(q, _):
        for t in range(2):
            acc = eus[t]
            for h in range(2):
                pick = one_hot(ids[pl.ds(pc.r * 2 + t, 1), :] - (q * 2 + h) * USERS, USERS)
                acc = acc + jnp.dot(eall[q, h * D:(h + 1) * D, :], pick, preferred_element_type=F32)
            eus[t] = acc
        return 0

    diffs((pc.r,))
    gq.relay()
    gu_all.relay()
    gq.wait_mate()
    diffs((pc.mate, pc.xn, pc.yn))
    gq.last()
    gu_all.last()
    gq.wait_mates()
    gu_all.wait_mate()
    gu_all.wait_mates()
    diffs((pc.mate_x, pc.mate_y))
    gq.finish()
    diffs((pc.dg, pc.mate_d))
    swap = pc.to_z(dif, ur.at[1], zs.at[1, 0], zr.at[1, 0])
    swap.start()
    gu_all.finish()
    lax.fori_loop(0, ROWS, users, 0)
    for h in range(2):
        egat[pc.r, h * D:(h + 1) * D, :] = eus[h].astype(BF16)
    ge.start()
    mg[0] = pack_rows([jnp.sum(eus[h] * dif[h], axis=0, keepdims=True) for h in range(2)])
    mz = pc.to_z(mg.at[0], mg.at[1], zs.at[1, 3], zr.at[1, 3])
    mz.start()
    acc = pi.at[1]
    acc[:6] = jnp.zeros((6, D, SHARD), F32)
    mz.wait()
    margin = mg[0] + mg[1]
    cg[pc.r, 0] = -jax.nn.sigmoid(-margin) / BATCH
    cg[pc.r, 1] = jnp.maximum(-margin, 0.0) + jnp.log1p(jnp.exp(-jnp.abs(margin)))
    coefs = []
    for j in range(1, ROWS):
        own = cg.at[pc.r]
        coefs.append(pc.to_row(own, own, ds.at[j - 1], dr.at[j - 1], (pc.r + j) % ROWS))
        coefs[-1].start()
    swap.wait()
    two = 2 * USERS

    def lanes(q, h):
        return pl.ds(pl.multiple_of((q % 2) * two + h * USERS, USERS), USERS)

    def unit(q):
        return rd.at[0, q // 2, :, window(q % 2, two)]

    def unit_part(q, h):
        return rd.at[0, q // 2, h * HALF:(h + 1) * HALF, window(q % 2, two)]

    gv = Gather(pc, unit, unit_part, gs.at[4], gr.at[4])
    for h in range(2):
        rd[0, pc.r // 2, :, lanes(pc.r, h)] = unpack_row(cg[pc.r, 0], h) * (dif[h] + ur[1, h])
    ge.relay()
    gv.start()
    ge.last()
    ge.wait_mate()
    ge.wait_mates()
    ge.finish()
    for cp in coefs:
        cp.wait()
    item_base = pc.c * ITEMS + pc.r * SHARD

    def item_grads(q, total):
        for h in range(2):
            k = q * 2 + h
            v = split3(unpack_row(cg[q, 0], h) * egat[q, h * D:(h + 1) * D, :].astype(F32))
            pos = ids[pl.ds(role + k, 1), :] - item_base
            neg = ids[pl.ds(2 * role + k, 1), :] - item_base
            for n in range(0, SHARD, USERS):
                picks = [one_hot(pos - b, FOLD) - one_hot(neg - b, FOLD) for b in (n, n + FOLD)]
                part_g = lax.dot_general(v, jnp.concatenate(picks, axis=0), NT, preferred_element_type=F32)
                for j in range(3):
                    acc[j, :, n:n + USERS] += part_g[j * D:(j + 1) * D]
        return total + cg[q, 1]

    def user_grads(q, _):
        for t in range(2):
            w = split3(rd[0, q // 2, :, lanes(q, t)])
            for h in range(2):
                pick = one_hot(ids[pl.ds(q * 2 + t, 1), :] - (pc.r * 2 + h) * USERS, USERS)
                part_g = lax.dot_general(w, pick, NT, preferred_element_type=F32)
                for j in range(3):
                    acc[3 + j, :, h * USERS:(h + 1) * USERS] += part_g[j * D:(j + 1) * D]
        return 0

    total = lax.fori_loop(0, 4, item_grads, jnp.zeros((ROWS, GROUP), F32))
    gv.relay()
    total = lax.fori_loop(4, 7, item_grads, total)
    gv.last()
    total = lax.fori_loop(7, ROWS, item_grads, total)
    whole = jnp.sum(jnp.sum(total, axis=0, keepdims=True), axis=1, keepdims=True)
    loss[...] = jnp.broadcast_to(whole / BATCH, loss.shape)
    src_i, src_u = acci, accu
    src_i[...] = ((acc[0] + acc[1]) + acc[2]) / (LAYERS + 1)
    gv.wait_mate()
    gv.wait_mates()
    gv.finish()

    objs['xis'], objs['gath'] = objs['xis'][::-1], objs['gath'][::-1]
    gp, gq = objs['gath']
    xi1[pc.r] = src_i[...].astype(BF16)
    gp.start()
    lax.fori_loop(0, ROWS, user_grads, 0)
    for h in range(2):
        there = slice(h * USERS, (h + 1) * USERS)
        src_u[h] = ((acc[3, :, there] + acc[4, :, there]) + acc[5, :, there]) / (LAYERS + 1)
        xu[0, h] = src_u[h].astype(BF16)

    def back_u(k, h, total):
        value = src_u[h] + total
        if k == LAYERS:
            @pl.when(pc.c == h)
            def _():
                gu[...] = value
        return value.astype(BF16)

    def back_i(k, rows, total):
        value = src_i[rows] + total
        if k == LAYERS:
            gi[rows] = value
        return value.astype(BF16)

    propagate(fin_u=back_u, fin_i=back_i, gather_first=True, **objs)


def mega_call(mask_blk, u0, i0, ids):
    dma = pltpu.SemaphoreType.DMA
    vm = pl.BlockSpec(memory_space=pltpu.VMEM)
    hbm = pl.BlockSpec(memory_space=pl.ANY)
    i32 = jnp.int32
    shape = jax.ShapeDtypeStruct
    return pl.pallas_call(
        mega_kernel,
        name='mega',
        out_shape=(shape((D, USERS), BF16), shape((D, SHARD), BF16), shape((ROWS, GROUP), F32), shape((D, USERS), F32), shape((D, SHARD), F32)),
        in_specs=[hbm, vm, vm, vm],
        out_specs=(vm, vm, vm, vm, vm),
        scratch_shapes=comm_scratch() + [
            pltpu.VMEM((ROWS, ROWS, FOLD), i32),
            pltpu.VMEM((ROWS - 1, ROWS, ROWS, FOLD), i32),
            pltpu.VMEM((ROWS, 2 * USERS), i32),
            pltpu.VMEM((ROWS, 2 * USERS), i32),
            pltpu.VMEM((TWO, D, USERS), F32),
            pltpu.VMEM((D, SHARD), F32),
            pltpu.VMEM((ROWS, 2 * D, USERS), BF16),
            pltpu.VMEM((ROWS, 2 * D, USERS), BF16),
            pltpu.VMEM((ROWS, TWO, ROWS, GROUP), F32),
            pltpu.VMEM((TWO, ROWS, GROUP), F32),
            dma((ROWS,)), dma((ROWS,)),
        ],
        compiler_params=pltpu.CompilerParams(collective_id=0, has_side_effects=True, vmem_limit_bytes=VMEM_LIMIT),
    )(mask_blk, u0, i0, ids)


def solution(mesh):
    def local_fn(mask_blk, user_emb, item_emb, triples):
        ids = triples.T.reshape(3 * BATCH // USERS, USERS)
        eu, ei, loss, gu, gi = mega_call(mask_blk, user_emb.T, item_emb.T, ids)
        return eu.T, ei.T, loss[0, 0], gu.T, gi.T

    user_spec = P(('row', 'col'), None)
    item_spec = P(('col', 'row'), None)
    return jax.shard_map(local_fn, mesh=mesh, in_specs=(P('row', 'col'), user_spec, item_spec, P()), out_specs=(user_spec, item_spec, P(), user_spec, item_spec), check_vma=False)
```

```python
import functools

import jax
import jax.numpy as jnp
from jax import lax
from jax.experimental import pallas as pl
from jax.experimental.pallas import tpu as pltpu
from jax.sharding import PartitionSpec as P

LAYERS = 3
MESH = pl.DeviceIdType.MESH
F32 = jnp.float32
BF16 = jnp.bfloat16
VMEM_LIMIT = 67_043_328
NT = (((1,), (1,)), ((), ()))
NONE, ONE, TWO, THREE = range(4)
D = 64
HALF = D // 2
SHARD = 2048
USERS = 512
GROUP = 128
FOLD = 256
ROWS = 8
SLOTS = 12
BATCH = 8192
ITEMS = ROWS * SHARD
LO, HI = slice(0, HALF), slice(HALF, D)


def choose(j, values):
    out = values[-1]
    for k in range(len(values) - 1):
        out = jnp.where(j == k, values[k], out)
    return out


def window(k, size):
    return pl.ds(pl.multiple_of(k * size, size), size)


class Place:
    def __init__(self):
        r = lax.axis_index('row')
        c = lax.axis_index('col')
        core = r % 2
        x = (r // 2) % 2
        y = r // 4
        self.r, self.c, self.core = r, c, core
        self.mate = r + 1 - 2 * core
        self.xn = r + 2 - 4 * x
        self.yn = r + 4 - 8 * y
        self.dg = self.xn + 4 - 8 * y
        self.zc = 1 - c
        d = 1 - 2 * core
        self.mate_x, self.mate_y, self.mate_d = self.xn + d, self.yn + d, self.dg + d

    def to_row(self, src, dst, ssem, rsem, row):
        return pltpu.make_async_remote_copy(src_ref=src, dst_ref=dst, send_sem=ssem, recv_sem=rsem, device_id={'row': row}, device_id_type=MESH)

    def to_z(self, src, dst, ssem, rsem):
        return pltpu.make_async_remote_copy(src_ref=src, dst_ref=dst, send_sem=ssem, recv_sem=rsem, device_id={'col': self.zc}, device_id_type=MESH)


def entry_signals(pc):
    bar = pltpu.get_barrier_semaphore()
    for j in range(1, ROWS):
        pl.semaphore_signal(bar, inc=1, device_id={'row': (pc.r + j) % ROWS}, device_id_type=MESH)
    pl.semaphore_signal(bar, inc=1, device_id={'col': pc.zc}, device_id_type=MESH)


class Gather:
    def __init__(self, pc, unit, part, ssem, rsem):
        self.pc, self.unit, self.part = pc, unit, part
        self.ssem, self.rsem = ssem, rsem
        own = unit(pc.r)
        hops = [(own, pc.xn), (own, pc.yn), (own, pc.mate), (part(pc.xn, 0), pc.yn), (part(pc.yn, 1), pc.xn)]
        hops += [(unit(pc.xn), pc.mate), (unit(pc.yn), pc.mate), (unit(pc.dg), pc.mate)]
        self.hops = [pc.to_row(ref, ref, ssem.at[k], rsem.at[k], to) for k, (ref, to) in enumerate(hops)]

    def _recv(self, k, ref):
        self.pc.to_row(ref, ref, self.ssem.at[k], self.rsem.at[k], self.pc.mate).wait_recv()

    def start(self):
        for hop in self.hops[:3]:
            hop.start()

    def wait_mate(self):
        self._recv(2, self.unit(self.pc.mate))

    def relay(self):
        pc, hops = self.pc, self.hops
        self._recv(0, self.unit(pc.xn))
        hops[3].start()
        hops[5].start()
        self._recv(1, self.unit(pc.yn))
        hops[4].start()
        hops[6].start()

    def wait_mates(self):
        pc = self.pc
        self._recv(5, self.unit(pc.mate_x))
        self._recv(6, self.unit(pc.mate_y))

    def last(self):
        pc = self.pc
        self._recv(3, self.part(pc.dg, 0))
        self._recv(4, self.part(pc.dg, 1))
        self.hops[7].start()

    def finish(self):
        self._recv(7, self.unit(self.pc.mate_d))
        for hop in self.hops:
            hop.wait_send()


def whole_gather(pc, ref, ssem, rsem):
    half = ref.shape[1] // 2
    return Gather(pc, lambda q: ref.at[q], lambda q, h: ref.at[q, h * half:(h + 1) * half], ssem, rsem)


class Scatter:
    def __init__(self, pc, pi, rd, rx, ry, rz, ssem, rsem):
        self.pc, self.pi = pc, pi
        self.rd, self.rx, self.ry, self.rz = rd, rx, ry, rz
        self.ssem, self.rsem = ssem, rsem
        self.mates = (pc.mate_d, pc.mate_x, pc.mate_y, pc.mate)
        self.owns = (pc.dg, pc.xn, pc.yn, pc.r)
        hops = [(pi.at[q], rd.at[k], pc.mate) for k, q in enumerate(self.mates)]
        hops += [(pi.at[pc.dg, LO], rx.at[1], pc.xn), (pi.at[pc.dg, HI], ry.at[1], pc.yn)]
        hops += [(pi.at[pc.xn, LO], rx.at[0], pc.xn), (pi.at[pc.yn, HI], ry.at[0], pc.yn)]
        hops += [(pi.at[pc.yn, LO], rz.at[0], pc.yn), (pi.at[pc.xn, HI], rz.at[1], pc.xn)]
        self.hops = [pc.to_row(src, dst, ssem.at[k], rsem.at[k], to) for k, (src, dst, to) in enumerate(hops)]
        self.far = self.hops[4:6]
        self.near = self.hops[6:8]
        self.late = self.hops[8:]

    def item(self, a, xu, send_far=True, send_near=True, between=None):
        pc, pi = self.pc, self.pi
        x = jnp.concatenate([xu[0], xu[1]], axis=1)
        blocks = [slice(n, n + USERS) for n in range(0, SHARD, USERS)]

        def for_mate(j):
            q = choose(j, self.mates)
            for n in blocks:
                pi[q, :, n] = jnp.dot(x, a[q, :, n], preferred_element_type=F32)
            pc.to_row(pi.at[q], self.rd.at[j], self.ssem.at[j], self.rsem.at[j], pc.mate).start()

        def for_self(j):
            q = choose(j, self.owns)
            pc.to_row(pi.at[q], self.rd.at[j], self.ssem.at[j], self.rsem.at[j], pc.mate).wait_recv()
            for n in blocks:
                pi[q, :, n] = self.rd[j, :, n] + jnp.dot(x, a[q, :, n], preferred_element_type=F32)

        def both(j, _):
            for_mate(j + 1)
            if between is not None:
                @pl.when(j == 1)
                def _():
                    between()
            for_self(j)
            if send_far:
                @pl.when(j == 0)
                def _():
                    self.start_far()
            if send_near:
                for k in range(2):
                    @pl.when(j == k + 1)
                    def _(k=k):
                        self.near[k].start()
            return 0

        for_mate(0)
        lax.fori_loop(0, 3, both, 0)
        for_self(3)

    def start_far(self):
        for hop in self.far:
            hop.start()

    def start_near(self):
        for hop in self.near:
            hop.start()

    def second(self):
        pc, pi = self.pc, self.pi
        self.far[0].wait_recv()
        pi[pc.yn, LO] += self.rx[1]
        self.late[0].start()
        self.far[1].wait_recv()
        pi[pc.xn, HI] += self.ry[1]
        self.late[1].start()

    def result(self, emit):
        pc, pi = self.pc, self.pi
        self.near[0].wait_recv()
        self.near[1].wait_recv()
        self.late[0].wait_recv()
        emit(LO, pi[pc.r, LO] + self.rx[0] + self.rz[0])
        self.late[1].wait_recv()
        emit(HI, pi[pc.r, HI] + self.ry[0] + self.rz[1])
        for hop in self.hops:
            hop.wait_send()


def user_part(a, xi, up, shards, first=False):
    if first:
        up[...] = jnp.zeros_like(up)

    def body(j, _):
        q = choose(j, shards)
        for h in range(2):
            up[h] += lax.dot_general(xi[q], a[q, h * USERS:(h + 1) * USERS, :], NT, preferred_element_type=F32)
        return 0

    lax.fori_loop(0, len(shards), body, 0)


def user_quarter(a, xi, up, shards, k):
    there = window(k % 2, FOLD)

    def body(j, _):
        q = choose(j, shards)
        up[k // 2, :, there] += lax.dot_general(xi[q], a[q, window(k, FOLD), :], NT, preferred_element_type=F32)
        return 0

    lax.fori_loop(0, len(shards), body, 0)


def propagate(pc, a, xis, xus, ups, urs, scat, gath, zs, zr, fin_u, fin_i, gather_first=False, after_u3=None):
    me = pc
    sp, sq = scat
    gp, gq = gath
    near = (me.r, me.mate, me.xn, me.yn)
    far = (me.mate_x, me.mate_y, me.dg, me.mate_d)

    def swap(ch, k):
        there = (k // 2, slice(None), window(k % 2, FOLD))
        return me.to_z(ups[ch].at[there], urs[ch].at[there], zs.at[ch, k], zr.at[ch, k])

    def send_users(ch, shards):
        def body(k, _):
            user_quarter(a, xis[ch], ups[ch], shards, k)
            swap(ch, k).start()
            return 0

        lax.fori_loop(0, 4, body, 0)

    def join_users(ch, k, xu):
        for h in range(2):
            swap(ch, 2 * h).wait()
            swap(ch, 2 * h + 1).wait()
            nxt = fin_u(k, h, ups[ch][h] + urs[ch][h])
            if xu is not None:
                xu[h] = nxt

    sq.item(a, xus[0], between=gp.relay if gather_first else None)
    if gather_first:
        gp.wait_mate()
    user_part(a, xis[0], ups[0], near, True)
    if gather_first:
        gp.last()
        gp.wait_mates()
        gp.finish()
    sq.second()
    send_users(0, far)

    def keep1(rows, value):
        xis[1][me.r, rows] = fin_i(1, rows, value)

    sq.result(keep1)
    gq.start()
    join_users(0, 1, xus[1])
    sp.item(a, xus[1], send_far=False, send_near=False)
    gq.relay()
    sp.start_far()
    sp.start_near()
    gq.wait_mate()
    user_part(a, xis[1], ups[1], near, True)
    gq.last()
    gq.wait_mates()
    user_part(a, xis[1], ups[1], far[:2])
    gq.finish()
    send_users(1, far[2:])
    sp.second()
    join_users(1, 2, xus[2])

    def keep2(rows, value):
        xis[0][me.r, rows] = fin_i(2, rows, value)

    def next_gather():
        sp.result(keep2)
        gp.start()

    sq.item(a, xus[2], send_near=False, between=next_gather)
    user_part(a, xis[0], ups[0], near[:1], True)
    gp.relay()
    sq.start_near()
    gp.wait_mate()
    user_part(a, xis[0], ups[0], near[1:])
    sq.second()
    gp.last()
    gp.wait_mates()
    user_part(a, xis[0], ups[0], far[:2])
    gp.finish()
    send_users(0, far[2:])
    join_users(0, 3, None)
    if after_u3 is not None:
        after_u3()

    def keep3(rows, value):
        fin_i(3, rows, value)

    sq.result(keep3)


def comm_scratch():
    dma = pltpu.SemaphoreType.DMA
    return [
        pltpu.VMEM((ROWS, 2 * USERS, SHARD), BF16),
        pltpu.VMEM((TWO, ROWS, D, SHARD), BF16),
        pltpu.VMEM((THREE, TWO, D, USERS), BF16),
        pltpu.VMEM((TWO, TWO, D, USERS), F32),
        pltpu.VMEM((TWO, TWO, D, USERS), F32),
        pltpu.VMEM((TWO, 4, D, SHARD), F32),
        pltpu.VMEM((TWO, 6, HALF, SHARD), F32),
        dma((5, ROWS)), dma((5, ROWS)), dma((TWO, 10)), dma((TWO, 10)), dma((TWO, 5)), dma((TWO, 5)),
    ]


def comm_objects(pc, pi, a, xi, xu, up, ur, rd, rxyz, gs, gr, ss, sr, zs, zr):
    scat = [Scatter(pc, pi.at[k], rd.at[k], rxyz.at[k, 0:2], rxyz.at[k, 2:4], rxyz.at[k, 4:6], ss.at[k], sr.at[k]) for k in range(2)]
    gath = [whole_gather(pc, xi.at[k], gs.at[k], gr.at[k]) for k in range(2)]
    return dict(pc=pc, a=a, xis=[xi.at[0], xi.at[1]], xus=[xu.at[k] for k in range(3)], ups=[up.at[0], up.at[1]],
                urs=[ur.at[0], ur.at[1]], scat=scat, gath=gath, zs=zs, zr=zr)


def one_hot(ids, rows):
    shape = (rows, ids.shape[1])
    wide = jnp.broadcast_to(ids.astype(jnp.int16), shape)
    return jnp.where(wide == lax.broadcasted_iota(jnp.int16, shape, 0), jnp.ones((), BF16), jnp.zeros((), BF16))


def split3(v):
    v1 = v.astype(BF16)
    rest = v - v1.astype(F32)
    v2 = rest.astype(BF16)
    v3 = (rest - v2.astype(F32)).astype(BF16)
    return jnp.concatenate([v1, v2, v3], axis=0)


def mega_kernel(m_hbm, u0, i0, ids, eu, ei, loss, gu, gi, *scratch):
    comm, rest = scratch[:13], scratch[13:]
    pc = Place()
    i32 = jnp.int32

    def first(stage, rowacc, colacc, sib, su, msem):
        form_adjacency(pc, m_hbm, u0, i0, comm, rest, stage, rowacc, colacc, sib, su, msem)

    pl.run_scoped(
        first,
        pltpu.VMEM((SLOTS, GROUP, SHARD), i32), pltpu.VMEM((2 * USERS, GROUP), i32), pltpu.VMEM((ROWS, SHARD), i32),
        pltpu.VMEM((ROWS, SHARD), F32), pltpu.VMEM((2 * USERS, GROUP), F32), pltpu.SemaphoreType.DMA((SLOTS,)),
    )
    pl.run_scoped(lambda pi: chains(pc, pi, ids, eu, ei, loss, gu, gi, comm, rest), pltpu.VMEM((TWO, ROWS, D, SHARD), F32))


def z_share(pc, ref, ssem, rsem):
    cp = pc.to_z(ref, ref, ssem, rsem)
    cp.start()
    return cp


def form_adjacency(pc, m_hbm, u0, i0, comm, rest, stage, rowacc, colacc, sib, su, msem):
    dpi, drecv, du, dur, accu, acci = rest[:6]
    ds, dr = rest[-2:]
    a, xi, xu = comm[:3]
    zs, zr = comm[11:]
    xi0 = xi.at[0]
    gp = whole_gather(pc, xi0, comm[7].at[0], comm[8].at[0])

    per_shard = 2 * USERS // GROUP

    def fetch(k):
        block = m_hbm.at[window(k % per_shard, GROUP), window(k // per_shard, SHARD)]
        return pltpu.make_async_copy(block, stage.at[k % SLOTS], msem.at[k % SLOTS])

    for k in range(SLOTS):
        fetch(k).start()
    xi0[pc.r] = i0[...]
    xu[0, pc.c] = u0[...]
    acci[...] = i0[...].astype(F32)
    rowacc[...] = jnp.zeros_like(rowacc)
    entry_signals(pc)
    strip = 2 * ROWS

    def degree_copy(j, q):
        return pc.to_row(dpi.at[q], drecv.at[j - 1, q], ds.at[j - 1], dr.at[j - 1], (pc.r + j) % ROWS)

    def shard(q, _):
        colacc[...] = jnp.zeros_like(colacc)

        def block(t, _):
            k = q * per_shard + t
            slot = k % SLOTS
            fetch(k).wait()

            def rows16(g, cols):
                here = window(g, strip)
                there = pl.ds(pl.multiple_of(t * GROUP + g * strip, strip), strip)
                racc = rowacc[there, :]
                out = []
                for n in range(0, SHARD, GROUP):
                    m = stage[slot, here, n:n + GROUP]
                    a[q, there, n:n + GROUP] = m.astype(F32).astype(BF16)
                    out.append(cols[n // GROUP] + (m[:ROWS] + m[ROWS:]))
                    racc = racc + m
                rowacc[there, :] = racc
                return tuple(out)

            lanes = range(0, SHARD, GROUP)
            cols = lax.fori_loop(0, GROUP // strip, rows16, tuple(colacc[:, n:n + GROUP] for n in lanes))
            for n, col in zip(lanes, cols):
                colacc[:, n:n + GROUP] = col

            @pl.when(k + SLOTS < ROWS * per_shard)
            def _():
                fetch(k + SLOTS).start()

            return 0

        lax.fori_loop(0, per_shard, block, 0)
        sums = jnp.sum(colacc[...], axis=0, keepdims=True)
        for s in range(ROWS):
            dpi[q, s:s + 1, :] = sums[:, s * FOLD:(s + 1) * FOLD]
        return 0

    def send_degrees(q):
        for j in range(1, ROWS):
            degree_copy(j, q).start()

    def shard_and_send(q, _):
        shard(q, 0)
        send_degrees(q)
        return 0

    lax.fori_loop(0, 2, shard, 0)
    pl.semaphore_wait(pltpu.get_barrier_semaphore(), ROWS)
    gp.start()
    share0 = z_share(pc, xu.at[0, pc.c], zs.at[0, 4], zr.at[0, 4])
    for q in range(2):
        send_degrees(q)
    lax.fori_loop(2, 5, shard_and_send, 0)
    gp.relay()
    lax.fori_loop(5, 7, shard_and_send, 0)
    gp.last()
    gp.wait_mate()
    gp.wait_mates()
    lax.fori_loop(7, ROWS, shard_and_send, 0)
    sums = jnp.sum(rowacc[...].astype(F32).T, axis=0, keepdims=True)
    du[...] = jnp.broadcast_to(sums, du.shape).astype(jnp.int32)
    zc = pc.to_z(du, dur, ds.at[ROWS - 1], dr.at[ROWS - 1])
    zc.start()
    gp.finish()
    share0.wait()
    accu[...] = xu[0].astype(F32)
    zc.wait()
    scale = lax.rsqrt(jnp.maximum(du[...] + dur[...], 1).astype(F32))
    su[...] = jnp.broadcast_to(scale[:1], (GROUP, 2 * USERS)).T
    for j in range(1, ROWS):
        whole = pc.to_row(dpi, drecv.at[j - 1], ds.at[j - 1], dr.at[j - 1], (pc.r + j) % ROWS)
        whole.wait()

    def form(q, _):
        deg = dpi[q]
        for j in range(ROWS - 1):
            deg = deg + drecv[j, q]
        scale = lax.rsqrt(jnp.maximum(deg, 1).astype(F32))
        for s in range(ROWS):
            sib[:, s * FOLD:(s + 1) * FOLD] = jnp.broadcast_to(scale[s:s + 1], (ROWS, FOLD))
        tall = ROWS * ROWS

        def rows64(t, _):
            rows = window(t, tall)
            sub = su[rows, :]
            sub = jnp.concatenate([sub, sub], axis=1)
            for n in range(0, SHARD, FOLD):
                col = sib[:, n:n + FOLD]
                both = (sub * jnp.concatenate([col] * ROWS, axis=0)).astype(BF16)
                a[q, rows, n:n + FOLD] = a[q, rows, n:n + FOLD] * both
            return 0

        lax.fori_loop(0, 2 * USERS // tall, rows64, 0)
        return 0

    lax.fori_loop(0, ROWS, form, 0)


def pack_rows(x):
    return jnp.concatenate([row[:, n:n + GROUP] for row in x for n in range(0, USERS, GROUP)], axis=0)


def unpack_row(tile, h):
    rows = USERS // GROUP
    return jnp.concatenate([tile[k:k + 1] for k in range(h * rows, (h + 1) * rows)], axis=1)


def chains(pc, pi, ids, eu, ei, loss, gu, gi, comm, rest):
    _, _, _, _, accu, acci, eall, egat, cg, mg, ds, dr = rest
    objs = comm_objects(pc, pi, *comm)
    a, xi, xu, up, ur, rd = comm[:6]
    gs, gr = comm[7:9]
    zs, zr = comm[11:]
    xi1 = xi.at[1]
    gp, gq = objs['gath']

    def fin_u(k, h, total):
        nxt = total.astype(BF16)
        accu[h] += nxt.astype(F32)
        return nxt

    def fin_i(k, rows, total):
        nxt = total.astype(BF16)
        acci[rows] += nxt.astype(F32)
        return nxt

    def named(role, chunk):
        return ids[role:role + 1, window(chunk, USERS)]

    gu_all = whole_gather(pc, eall, gs.at[2], gr.at[2])
    ge = whole_gather(pc, egat, gs.at[3], gr.at[3])

    def after_u3():
        for h in range(2):
            eall[pc.r, h * D:(h + 1) * D, :] = (accu[h] / (LAYERS + 1)).astype(BF16)
        gu_all.start()

    propagate(fin_u=fin_u, fin_i=fin_i, after_u3=after_u3, **objs)

    e = (acci[...] / (LAYERS + 1)).astype(BF16)
    xi1[pc.r] = e
    gq.start()
    ei[...] = e
    eu[...] = (accu[pc.c] / (LAYERS + 1)).astype(BF16)

    dif, eus = up.at[0], up.at[1]
    dif[...] = jnp.zeros_like(dif)
    eus[...] = jnp.zeros_like(eus)

    def diffs(shards):
        def body(j, _):
            q, h = choose(j // 2, shards), j % 2
            base = pc.c * ITEMS + q * SHARD
            pos = named(1, pc.r * 2 + h) - base
            neg = named(2, pc.r * 2 + h) - base
            acc = dif[h]
            for s in range(0, SHARD, FOLD):
                pick = one_hot(pos - s, FOLD) - one_hot(neg - s, FOLD)
                acc = acc + jnp.dot(xi1[q, :, s:s + FOLD], pick, preferred_element_type=F32)
            dif[h] = acc
            return 0

        lax.fori_loop(0, 2 * len(shards), body, 0)

    def users(shards):
        def body(j, _):
            q, t = choose(j // 2, shards), j % 2
            acc = eus[t]
            for h in range(2):
                pick = one_hot(named(0, pc.r * 2 + t) - (q * 2 + h) * USERS, USERS)
                acc = acc + jnp.dot(eall[q, h * D:(h + 1) * D, :], pick, preferred_element_type=F32)
            eus[t] = acc
            return 0

        lax.fori_loop(0, 2 * len(shards), body, 0)

    gu_all.relay()
    diffs((pc.r,))
    gu_all.wait_mate()
    users((pc.r, pc.mate, pc.xn, pc.yn))
    gu_all.last()
    gq.relay()
    gu_all.wait_mates()
    gu_all.finish()
    users((pc.mate_x, pc.mate_y, pc.dg, pc.mate_d))
    for h in range(2):
        egat[pc.r, h * D:(h + 1) * D, :] = eus[h].astype(BF16)
    ge.start()
    gq.wait_mate()
    diffs((pc.mate, pc.xn, pc.yn))
    gq.last()
    gq.wait_mates()
    diffs((pc.mate_x, pc.mate_y))
    ge.relay()
    gq.finish()
    diffs((pc.dg, pc.mate_d))
    swap = pc.to_z(dif, ur.at[1], zs.at[1, 0], zr.at[1, 0])
    mg[0] = pack_rows([jnp.sum(eus[h] * dif[h], axis=0, keepdims=True) for h in range(2)])
    mz = pc.to_z(mg.at[0], mg.at[1], zs.at[1, 4], zr.at[1, 4])
    mz.start()
    swap.start()
    ge.last()
    acc = pi.at[1]
    acc[:6] = jnp.zeros((6, D, SHARD), F32)
    mz.wait()
    margin = mg[0] + mg[1]
    cg[pc.r, 0] = -jax.nn.sigmoid(-margin) / BATCH
    cg[pc.r, 1] = jnp.maximum(-margin, 0.0) + jnp.log1p(jnp.exp(-jnp.abs(margin)))
    coefs = []
    for j in range(1, ROWS):
        own = cg.at[pc.r]
        coefs.append(pc.to_row(own, own, ds.at[j - 1], dr.at[j - 1], (pc.r + j) % ROWS))
        coefs[-1].start()
    swap.wait()
    two = 2 * USERS

    def lanes(q, h):
        return pl.ds(pl.multiple_of((q % 2) * two + h * USERS, USERS), USERS)

    def unit(q):
        return rd.at[0, q // 2, :, window(q % 2, two)]

    def unit_part(q, h):
        return rd.at[0, q // 2, h * HALF:(h + 1) * HALF, window(q % 2, two)]

    gv = Gather(pc, unit, unit_part, gs.at[4], gr.at[4])
    for h in range(2):
        rd[0, pc.r // 2, :, lanes(pc.r, h)] = unpack_row(cg[pc.r, 0], h) * (dif[h] + ur[1, h])
    gv.start()
    ge.wait_mate()
    ge.wait_mates()
    ge.finish()
    for cp in coefs:
        cp.wait()
    item_base = pc.c * ITEMS + pc.r * SHARD

    def item_grads(q, total):
        for h in range(2):
            k = q * 2 + h
            v = split3(unpack_row(cg[q, 0], h) * egat[q, h * D:(h + 1) * D, :].astype(F32))
            pos = named(1, k) - item_base
            neg = named(2, k) - item_base
            for n in range(0, SHARD, USERS):
                picks = [one_hot(pos - b, FOLD) - one_hot(neg - b, FOLD) for b in (n, n + FOLD)]
                part_g = lax.dot_general(v, jnp.concatenate(picks, axis=0), NT, preferred_element_type=F32)
                for j in range(3):
                    acc[j, :, n:n + USERS] += part_g[j * D:(j + 1) * D]
        return total + cg[q, 1]

    def user_grads(q, _):
        for t in range(2):
            w = split3(rd[0, q // 2, :, lanes(q, t)])
            for h in range(2):
                pick = one_hot(named(0, q * 2 + t) - (pc.r * 2 + h) * USERS, USERS)
                part_g = lax.dot_general(w, pick, NT, preferred_element_type=F32)
                for j in range(3):
                    acc[3 + j, :, h * USERS:(h + 1) * USERS] += part_g[j * D:(j + 1) * D]
        return 0

    total = lax.fori_loop(0, 4, item_grads, jnp.zeros((ROWS, GROUP), F32))
    gv.relay()
    total = lax.fori_loop(4, 7, item_grads, total)
    gv.last()
    total = lax.fori_loop(7, ROWS, item_grads, total)
    whole = jnp.sum(jnp.sum(total, axis=0, keepdims=True), axis=1, keepdims=True)
    loss[...] = whole / BATCH
    src_i, src_u = acci, accu
    src_i[...] = ((acc[0] + acc[1]) + acc[2]) / (LAYERS + 1)
    gv.wait_mate()
    gv.wait_mates()
    gv.finish()

    objs['xis'], objs['gath'] = objs['xis'][::-1], objs['gath'][::-1]
    gp, gq = objs['gath']
    xi1[pc.r] = src_i[...].astype(BF16)
    gp.start()
    lax.fori_loop(0, ROWS, user_grads, 0)
    for h in range(2):
        there = slice(h * USERS, (h + 1) * USERS)
        src_u[h] = ((acc[3, :, there] + acc[4, :, there]) + acc[5, :, there]) / (LAYERS + 1)
        xu[0, h] = src_u[h].astype(BF16)

    def back_u(k, h, total):
        value = src_u[h] + total
        if k == LAYERS:
            @pl.when(pc.c == h)
            def _():
                gu[...] = value
        return value.astype(BF16)

    def back_i(k, rows, total):
        value = src_i[rows] + total
        if k == LAYERS:
            gi[rows] = value
        return value.astype(BF16)

    propagate(fin_u=back_u, fin_i=back_i, gather_first=True, **objs)


def mega_call(mask_blk, u0, i0, ids):
    dma = pltpu.SemaphoreType.DMA
    vm = pl.BlockSpec(memory_space=pltpu.VMEM)
    hbm = pl.BlockSpec(memory_space=pl.ANY)
    i32 = jnp.int32
    shape = jax.ShapeDtypeStruct
    return pl.pallas_call(
        mega_kernel,
        name='mega',
        out_shape=(shape((D, USERS), BF16), shape((D, SHARD), BF16), shape((1, 1), F32), shape((D, USERS), F32), shape((D, SHARD), F32)),
        in_specs=[hbm, vm, vm, vm],
        out_specs=(vm, vm, vm, vm, vm),
        scratch_shapes=comm_scratch() + [
            pltpu.VMEM((ROWS, ROWS, FOLD), i32),
            pltpu.VMEM((ROWS - 1, ROWS, ROWS, FOLD), i32),
            pltpu.VMEM((ROWS, 2 * USERS), i32),
            pltpu.VMEM((ROWS, 2 * USERS), i32),
            pltpu.VMEM((TWO, D, USERS), F32),
            pltpu.VMEM((D, SHARD), F32),
            pltpu.VMEM((ROWS, 2 * D, USERS), BF16),
            pltpu.VMEM((ROWS, 2 * D, USERS), BF16),
            pltpu.VMEM((ROWS, TWO, ROWS, GROUP), F32),
            pltpu.VMEM((TWO, ROWS, GROUP), F32),
            dma((ROWS,)), dma((ROWS,)),
        ],
        compiler_params=pltpu.CompilerParams(collective_id=0, has_side_effects=True, vmem_limit_bytes=VMEM_LIMIT),
    )(mask_blk, u0, i0, ids)


def settle_kernel(*refs):
    half = len(refs) // 2
    for src, dst in zip(refs[:half], refs[half:]):
        dst[...] = src[...]


def settle_call(*arrays):
    shapes = tuple(jax.ShapeDtypeStruct(x.shape, x.dtype) for x in arrays)
    return pl.pallas_call(settle_kernel, name='settle', out_shape=shapes)(*arrays)


def solution(mesh):
    def local_fn(mask_blk, user_emb, item_emb, triples):
        eu, ei, loss, gu, gi = settle_call(*mega_call(mask_blk, user_emb.T, item_emb.T, triples.T))
        return eu.T, ei.T, loss.reshape(()), gu.T, gi.T

    user_spec = P(('row', 'col'), None)
    item_spec = P(('col', 'row'), None)
    return jax.shard_map(local_fn, mesh=mesh, in_specs=(P('row', 'col'), user_spec, item_spec, P()), out_specs=(user_spec, item_spec, P(), user_spec, item_spec), check_vma=False)
```

```python
import functools

import jax
import jax.numpy as jnp
from jax import lax
from jax.experimental import pallas as pl
from jax.experimental.pallas import tpu as pltpu
from jax.sharding import PartitionSpec as P

LAYERS = 3
MESH = pl.DeviceIdType.MESH
F32 = jnp.float32
BF16 = jnp.bfloat16
VMEM_LIMIT = 67_043_328
NT = (((1,), (1,)), ((), ()))
NONE, ONE, TWO, THREE = range(4)
D = 64
HALF = D // 2
SHARD = 2048
USERS = 512
GROUP = 128
FOLD = 256
ROWS = 8
SLOTS = 12
BATCH = 8192
ITEMS = ROWS * SHARD
LO, HI = slice(0, HALF), slice(HALF, D)


def choose(j, values):
    out = values[-1]
    for k in range(len(values) - 1):
        out = jnp.where(j == k, values[k], out)
    return out


def window(k, size):
    return pl.ds(pl.multiple_of(k * size, size), size)


class Place:
    def __init__(self):
        r = lax.axis_index('row')
        c = lax.axis_index('col')
        core = r % 2
        x = (r // 2) % 2
        y = r // 4
        self.r, self.c, self.core = r, c, core
        self.mate = r + 1 - 2 * core
        self.xn = r + 2 - 4 * x
        self.yn = r + 4 - 8 * y
        self.dg = self.xn + 4 - 8 * y
        self.zc = 1 - c
        d = 1 - 2 * core
        self.mate_x, self.mate_y, self.mate_d = self.xn + d, self.yn + d, self.dg + d

    def to_row(self, src, dst, ssem, rsem, row):
        return pltpu.make_async_remote_copy(src_ref=src, dst_ref=dst, send_sem=ssem, recv_sem=rsem, device_id={'row': row}, device_id_type=MESH)

    def to_z(self, src, dst, ssem, rsem):
        return pltpu.make_async_remote_copy(src_ref=src, dst_ref=dst, send_sem=ssem, recv_sem=rsem, device_id={'col': self.zc}, device_id_type=MESH)


def entry_signals(pc):
    bar = pltpu.get_barrier_semaphore()
    for j in range(1, ROWS):
        pl.semaphore_signal(bar, inc=1, device_id={'row': (pc.r + j) % ROWS}, device_id_type=MESH)
    pl.semaphore_signal(bar, inc=1, device_id={'col': pc.zc}, device_id_type=MESH)


class Gather:
    def __init__(self, pc, unit, part, ssem, rsem):
        self.pc, self.unit, self.part = pc, unit, part
        self.ssem, self.rsem = ssem, rsem
        own = unit(pc.r)
        hops = [(own, pc.xn), (own, pc.yn), (own, pc.mate), (part(pc.xn, 0), pc.yn), (part(pc.yn, 1), pc.xn)]
        hops += [(unit(pc.xn), pc.mate), (unit(pc.yn), pc.mate), (unit(pc.dg), pc.mate)]
        self.hops = [pc.to_row(ref, ref, ssem.at[k], rsem.at[k], to) for k, (ref, to) in enumerate(hops)]

    def _recv(self, k, ref):
        self.pc.to_row(ref, ref, self.ssem.at[k], self.rsem.at[k], self.pc.mate).wait_recv()

    def start(self):
        for hop in self.hops[:3]:
            hop.start()

    def wait_mate(self):
        self._recv(2, self.unit(self.pc.mate))

    def relay(self):
        pc, hops = self.pc, self.hops
        self._recv(0, self.unit(pc.xn))
        hops[3].start()
        hops[5].start()
        self._recv(1, self.unit(pc.yn))
        hops[4].start()
        hops[6].start()

    def wait_mates(self):
        pc = self.pc
        self._recv(5, self.unit(pc.mate_x))
        self._recv(6, self.unit(pc.mate_y))

    def last(self):
        pc = self.pc
        self._recv(3, self.part(pc.dg, 0))
        self._recv(4, self.part(pc.dg, 1))
        self.hops[7].start()

    def finish(self):
        self._recv(7, self.unit(self.pc.mate_d))
        for hop in self.hops:
            hop.wait_send()


def whole_gather(pc, ref, ssem, rsem):
    half = ref.shape[1] // 2
    return Gather(pc, lambda q: ref.at[q], lambda q, h: ref.at[q, h * half:(h + 1) * half], ssem, rsem)


class Scatter:
    def __init__(self, pc, pi, rd, rx, ry, rz, ssem, rsem):
        self.pc, self.pi = pc, pi
        self.rd, self.rx, self.ry, self.rz = rd, rx, ry, rz
        self.ssem, self.rsem = ssem, rsem
        self.mates = (pc.mate_d, pc.mate_x, pc.mate_y, pc.mate)
        self.owns = (pc.dg, pc.xn, pc.yn, pc.r)
        hops = [(pi.at[q], rd.at[k], pc.mate) for k, q in enumerate(self.mates)]
        hops += [(pi.at[pc.dg, LO], rx.at[1], pc.xn), (pi.at[pc.dg, HI], ry.at[1], pc.yn)]
        hops += [(pi.at[pc.xn, LO], rx.at[0], pc.xn), (pi.at[pc.yn, HI], ry.at[0], pc.yn)]
        hops += [(pi.at[pc.yn, LO], rz.at[0], pc.yn), (pi.at[pc.xn, HI], rz.at[1], pc.xn)]
        self.hops = [pc.to_row(src, dst, ssem.at[k], rsem.at[k], to) for k, (src, dst, to) in enumerate(hops)]
        self.far = self.hops[4:6]
        self.near = self.hops[6:8]
        self.late = self.hops[8:]

    def item(self, a, xu, send_far=True, send_near=True, between=None):
        pc, pi = self.pc, self.pi
        x = jnp.concatenate([xu[0], xu[1]], axis=1)
        blocks = [slice(n, n + USERS) for n in range(0, SHARD, USERS)]

        def for_mate(j):
            q = choose(j, self.mates)
            for n in blocks:
                pi[q, :, n] = jnp.dot(x, a[q, :, n], preferred_element_type=F32)
            pc.to_row(pi.at[q], self.rd.at[j], self.ssem.at[j], self.rsem.at[j], pc.mate).start()

        def for_self(j):
            q = choose(j, self.owns)
            pc.to_row(pi.at[q], self.rd.at[j], self.ssem.at[j], self.rsem.at[j], pc.mate).wait_recv()
            for n in blocks:
                pi[q, :, n] = self.rd[j, :, n] + jnp.dot(x, a[q, :, n], preferred_element_type=F32)

        def both(j, _):
            for_mate(j + 1)
            if between is not None:
                @pl.when(j == 1)
                def _():
                    between()
            for_self(j)
            if send_far:
                @pl.when(j == 0)
                def _():
                    self.start_far()
            if send_near:
                for k in range(2):
                    @pl.when(j == k + 1)
                    def _(k=k):
                        self.near[k].start()
            return 0

        for_mate(0)
        lax.fori_loop(0, 3, both, 0)
        for_self(3)

    def start_far(self):
        for hop in self.far:
            hop.start()

    def start_near(self):
        for hop in self.near:
            hop.start()

    def second(self):
        pc, pi = self.pc, self.pi
        self.far[0].wait_recv()
        pi[pc.yn, LO] += self.rx[1]
        self.late[0].start()
        self.far[1].wait_recv()
        pi[pc.xn, HI] += self.ry[1]
        self.late[1].start()

    def result(self, emit):
        pc, pi = self.pc, self.pi
        self.near[0].wait_recv()
        self.near[1].wait_recv()
        self.late[0].wait_recv()
        emit(LO, pi[pc.r, LO] + self.rx[0] + self.rz[0])
        self.late[1].wait_recv()
        emit(HI, pi[pc.r, HI] + self.ry[0] + self.rz[1])
        for hop in self.hops:
            hop.wait_send()


def user_part(a, xi, up, shards, first=False):
    if first:
        up[...] = jnp.zeros_like(up)

    def body(j, _):
        q = choose(j, shards)
        for h in range(2):
            up[h] += lax.dot_general(xi[q], a[q, h * USERS:(h + 1) * USERS, :], NT, preferred_element_type=F32)
        return 0

    lax.fori_loop(0, len(shards), body, 0)


def user_quarter(a, xi, up, shards, k):
    there = window(k % 2, FOLD)

    def body(j, _):
        q = choose(j, shards)
        up[k // 2, :, there] += lax.dot_general(xi[q], a[q, window(k, FOLD), :], NT, preferred_element_type=F32)
        return 0

    lax.fori_loop(0, len(shards), body, 0)


def propagate(pc, a, xis, xus, ups, urs, scat, gath, zs, zr, fin_u, fin_i, gather_first=False, after_u3=None):
    me = pc
    sp, sq = scat
    gp, gq = gath
    near = (me.r, me.mate, me.xn, me.yn)
    far = (me.mate_x, me.mate_y, me.dg, me.mate_d)

    def swap(ch, k):
        there = (k // 2, slice(None), window(k % 2, FOLD))
        return me.to_z(ups[ch].at[there], urs[ch].at[there], zs.at[ch, k], zr.at[ch, k])

    def send_users(ch, shards):
        def body(k, _):
            user_quarter(a, xis[ch], ups[ch], shards, k)
            swap(ch, k).start()
            return 0

        lax.fori_loop(0, 4, body, 0)

    def join_users(ch, k, xu):
        for h in range(2):
            swap(ch, 2 * h).wait()
            swap(ch, 2 * h + 1).wait()
            nxt = fin_u(k, h, ups[ch][h] + urs[ch][h])
            if xu is not None:
                xu[h] = nxt

    sq.item(a, xus[0], between=gp.relay if gather_first else None)
    if gather_first:
        gp.wait_mate()
    user_part(a, xis[0], ups[0], near, True)
    if gather_first:
        gp.last()
        gp.wait_mates()
        gp.finish()
    sq.second()
    send_users(0, far)

    def keep1(rows, value):
        xis[1][me.r, rows] = fin_i(1, rows, value)

    sq.result(keep1)
    gq.start()
    join_users(0, 1, xus[1])
    sp.item(a, xus[1], send_far=False, send_near=False)
    gq.relay()
    sp.start_far()
    sp.start_near()
    gq.wait_mate()
    user_part(a, xis[1], ups[1], near, True)
    gq.last()
    gq.wait_mates()
    user_part(a, xis[1], ups[1], far[:2])
    gq.finish()
    send_users(1, far[2:])
    sp.second()
    join_users(1, 2, xus[2])

    def keep2(rows, value):
        xis[0][me.r, rows] = fin_i(2, rows, value)

    def next_gather():
        sp.result(keep2)
        gp.start()

    sq.item(a, xus[2], send_near=False, between=next_gather)
    user_part(a, xis[0], ups[0], near[:1], True)
    gp.relay()
    sq.start_near()
    gp.wait_mate()
    user_part(a, xis[0], ups[0], near[1:])
    sq.second()
    gp.last()
    gp.wait_mates()
    user_part(a, xis[0], ups[0], far[:2])
    gp.finish()
    send_users(0, far[2:])
    join_users(0, 3, None)
    if after_u3 is not None:
        after_u3()

    def keep3(rows, value):
        fin_i(3, rows, value)

    sq.result(keep3)


def comm_scratch():
    dma = pltpu.SemaphoreType.DMA
    return [
        pltpu.VMEM((ROWS, 2 * USERS, SHARD), BF16),
        pltpu.VMEM((TWO, ROWS, D, SHARD), BF16),
        pltpu.VMEM((THREE, TWO, D, USERS), BF16),
        pltpu.VMEM((TWO, TWO, D, USERS), F32),
        pltpu.VMEM((TWO, TWO, D, USERS), F32),
        pltpu.VMEM((TWO, 4, D, SHARD), F32),
        pltpu.VMEM((TWO, 6, HALF, SHARD), F32),
        dma((5, ROWS)), dma((5, ROWS)), dma((TWO, 10)), dma((TWO, 10)), dma((TWO, 5)), dma((TWO, 5)),
    ]


def comm_objects(pc, pi, a, xi, xu, up, ur, rd, rxyz, gs, gr, ss, sr, zs, zr):
    scat = [Scatter(pc, pi.at[k], rd.at[k], rxyz.at[k, 0:2], rxyz.at[k, 2:4], rxyz.at[k, 4:6], ss.at[k], sr.at[k]) for k in range(2)]
    gath = [whole_gather(pc, xi.at[k], gs.at[k], gr.at[k]) for k in range(2)]
    return dict(pc=pc, a=a, xis=[xi.at[0], xi.at[1]], xus=[xu.at[k] for k in range(3)], ups=[up.at[0], up.at[1]],
                urs=[ur.at[0], ur.at[1]], scat=scat, gath=gath, zs=zs, zr=zr)


def one_hot(ids, rows):
    shape = (rows, ids.shape[1])
    wide = jnp.broadcast_to(ids.astype(jnp.int16), shape)
    return jnp.where(wide == lax.broadcasted_iota(jnp.int16, shape, 0), jnp.ones((), BF16), jnp.zeros((), BF16))


def split3(v):
    v1 = v.astype(BF16)
    rest = v - v1.astype(F32)
    v2 = rest.astype(BF16)
    v3 = (rest - v2.astype(F32)).astype(BF16)
    return jnp.concatenate([v1, v2, v3], axis=0)


def mega_kernel(m_hbm, u0, i0, ids, eu, ei, loss, gu, gi, *scratch):
    comm, rest = scratch[:13], scratch[13:]
    pc = Place()
    i32 = jnp.int32

    def first(stage, rowacc, colacc, sib, su, msem):
        form_adjacency(pc, m_hbm, u0, i0, comm, rest, stage, rowacc, colacc, sib, su, msem)

    pl.run_scoped(
        first,
        pltpu.VMEM((SLOTS, GROUP, SHARD), i32), pltpu.VMEM((2 * USERS, GROUP), i32), pltpu.VMEM((ROWS, SHARD), i32),
        pltpu.VMEM((ROWS, SHARD), F32), pltpu.VMEM((2 * USERS, GROUP), F32), pltpu.SemaphoreType.DMA((SLOTS,)),
    )
    pl.run_scoped(lambda pi: chains(pc, pi, ids, eu, ei, loss, gu, gi, comm, rest), pltpu.VMEM((TWO, ROWS, D, SHARD), F32))


def z_share(pc, ref, ssem, rsem):
    cp = pc.to_z(ref, ref, ssem, rsem)
    cp.start()
    return cp


def form_adjacency(pc, m_hbm, u0, i0, comm, rest, stage, rowacc, colacc, sib, su, msem):
    dpi, drecv, du, dur, accu, acci = rest[:6]
    ds, dr = rest[-2:]
    a, xi, xu = comm[:3]
    zs, zr = comm[11:]
    xi0 = xi.at[0]
    gp = whole_gather(pc, xi0, comm[7].at[0], comm[8].at[0])

    per_shard = 2 * USERS // GROUP

    def fetch(k):
        block = m_hbm.at[window(k % per_shard, GROUP), window(k // per_shard, SHARD)]
        return pltpu.make_async_copy(block, stage.at[k % SLOTS], msem.at[k % SLOTS])

    for k in range(SLOTS):
        fetch(k).start()
    xi0[pc.r] = i0[...]
    xu[0, pc.c] = u0[...]
    acci[...] = i0[...].astype(F32)
    rowacc[...] = jnp.zeros_like(rowacc)
    entry_signals(pc)
    strip = 2 * ROWS

    def degree_copy(j, q):
        return pc.to_row(dpi.at[q], drecv.at[j - 1, q], ds.at[j - 1], dr.at[j - 1], (pc.r + j) % ROWS)

    def shard(q, _):
        colacc[...] = jnp.zeros_like(colacc)

        def block(t, _):
            k = q * per_shard + t
            slot = k % SLOTS
            fetch(k).wait()

            def rows16(g, cols):
                here = window(g, strip)
                there = pl.ds(pl.multiple_of(t * GROUP + g * strip, strip), strip)
                racc = rowacc[there, :]
                out = []
                for n in range(0, SHARD, GROUP):
                    m = stage[slot, here, n:n + GROUP]
                    a[q, there, n:n + GROUP] = m.astype(F32).astype(BF16)
                    out.append(cols[n // GROUP] + (m[:ROWS] + m[ROWS:]))
                    racc = racc + m
                rowacc[there, :] = racc
                return tuple(out)

            lanes = range(0, SHARD, GROUP)
            cols = lax.fori_loop(0, GROUP // strip, rows16, tuple(colacc[:, n:n + GROUP] for n in lanes))
            for n, col in zip(lanes, cols):
                colacc[:, n:n + GROUP] = col

            @pl.when(k + SLOTS < ROWS * per_shard)
            def _():
                fetch(k + SLOTS).start()

            return 0

        lax.fori_loop(0, per_shard, block, 0)
        sums = jnp.sum(colacc[...], axis=0, keepdims=True)
        for s in range(ROWS):
            dpi[q, s:s + 1, :] = sums[:, s * FOLD:(s + 1) * FOLD]
        return 0

    def send_degrees(q):
        for j in range(1, ROWS):
            degree_copy(j, q).start()

    def shard_and_send(q, _):
        shard(q, 0)
        send_degrees(q)
        return 0

    lax.fori_loop(0, 2, shard, 0)
    pl.semaphore_wait(pltpu.get_barrier_semaphore(), ROWS)
    gp.start()
    share0 = z_share(pc, xu.at[0, pc.c], zs.at[0, 4], zr.at[0, 4])
    for q in range(2):
        send_degrees(q)
    lax.fori_loop(2, 5, shard_and_send, 0)
    gp.relay()
    lax.fori_loop(5, 7, shard_and_send, 0)
    gp.last()
    gp.wait_mate()
    gp.wait_mates()
    lax.fori_loop(7, ROWS, shard_and_send, 0)
    sums = jnp.sum(rowacc[...].astype(F32).T, axis=0, keepdims=True)
    du[...] = jnp.broadcast_to(sums, du.shape).astype(jnp.int32)
    zc = pc.to_z(du, dur, ds.at[ROWS - 1], dr.at[ROWS - 1])
    zc.start()
    gp.finish()
    share0.wait()
    accu[...] = xu[0].astype(F32)
    zc.wait()
    scale = lax.rsqrt(jnp.maximum(du[...] + dur[...], 1).astype(F32))
    su[...] = jnp.broadcast_to(scale[:1], (GROUP, 2 * USERS)).T
    for j in range(1, ROWS):
        whole = pc.to_row(dpi, drecv.at[j - 1], ds.at[j - 1], dr.at[j - 1], (pc.r + j) % ROWS)
        whole.wait()

    def form(q, _):
        deg = dpi[q]
        for j in range(ROWS - 1):
            deg = deg + drecv[j, q]
        scale = lax.rsqrt(jnp.maximum(deg, 1).astype(F32))
        for s in range(ROWS):
            sib[:, s * FOLD:(s + 1) * FOLD] = jnp.broadcast_to(scale[s:s + 1], (ROWS, FOLD))
        tall = ROWS * ROWS

        def rows64(t, _):
            rows = window(t, tall)
            sub = su[rows, :]
            sub = jnp.concatenate([sub, sub], axis=1)
            for n in range(0, SHARD, FOLD):
                col = sib[:, n:n + FOLD]
                both = (sub * jnp.concatenate([col] * ROWS, axis=0)).astype(BF16)
                a[q, rows, n:n + FOLD] = a[q, rows, n:n + FOLD] * both
            return 0

        lax.fori_loop(0, 2 * USERS // tall, rows64, 0)
        return 0

    lax.fori_loop(0, ROWS, form, 0)


def pack_rows(x):
    return jnp.concatenate([row[:, n:n + GROUP] for row in x for n in range(0, USERS, GROUP)], axis=0)


def unpack_row(tile, h):
    rows = USERS // GROUP
    return jnp.concatenate([tile[k:k + 1] for k in range(h * rows, (h + 1) * rows)], axis=1)


def chains(pc, pi, ids, eu, ei, loss, gu, gi, comm, rest):
    _, _, _, _, accu, acci, eall, egat, cg, mg, ds, dr = rest
    objs = comm_objects(pc, pi, *comm)
    a, xi, xu, up, ur, rd = comm[:6]
    gs, gr = comm[7:9]
    zs, zr = comm[11:]
    xi1 = xi.at[1]
    gp, gq = objs['gath']

    def fin_u(k, h, total):
        nxt = total.astype(BF16)
        accu[h] += nxt.astype(F32)
        return nxt

    def fin_i(k, rows, total):
        nxt = total.astype(BF16)
        acci[rows] += nxt.astype(F32)
        return nxt

    def named(role, chunk):
        return ids[role:role + 1, window(chunk, USERS)]

    gu_all = whole_gather(pc, eall, gs.at[2], gr.at[2])
    ge = whole_gather(pc, egat, gs.at[3], gr.at[3])

    def after_u3():
        for h in range(2):
            eall[pc.r, h * D:(h + 1) * D, :] = (accu[h] / (LAYERS + 1)).astype(BF16)
        gu_all.start()

    propagate(fin_u=fin_u, fin_i=fin_i, after_u3=after_u3, **objs)

    e = (acci[...] / (LAYERS + 1)).astype(BF16)
    xi1[pc.r] = e
    gq.start()
    ei[...] = e
    eu[...] = (accu[pc.c] / (LAYERS + 1)).astype(BF16)

    dif, eus = up.at[0], up.at[1]
    dif[...] = jnp.zeros_like(dif)
    eus[...] = jnp.zeros_like(eus)

    def diffs(shards):
        def body(j, _):
            q, h = choose(j // 2, shards), j % 2
            base = pc.c * ITEMS + q * SHARD
            pos = named(1, pc.r * 2 + h) - base
            neg = named(2, pc.r * 2 + h) - base
            acc = dif[h]
            for s in range(0, SHARD, FOLD):
                pick = one_hot(pos - s, FOLD) - one_hot(neg - s, FOLD)
                acc = acc + jnp.dot(xi1[q, :, s:s + FOLD], pick, preferred_element_type=F32)
            dif[h] = acc
            return 0

        lax.fori_loop(0, 2 * len(shards), body, 0)

    def users(shards):
        def body(j, _):
            q, t = choose(j // 2, shards), j % 2
            acc = eus[t]
            for h in range(2):
                pick = one_hot(named(0, pc.r * 2 + t) - (q * 2 + h) * USERS, USERS)
                acc = acc + jnp.dot(eall[q, h * D:(h + 1) * D, :], pick, preferred_element_type=F32)
            eus[t] = acc
            return 0

        lax.fori_loop(0, 2 * len(shards), body, 0)

    gu_all.relay()
    diffs((pc.r,))
    gu_all.wait_mate()
    users((pc.r, pc.mate, pc.xn, pc.yn))
    gu_all.last()
    gq.relay()
    gu_all.wait_mates()
    gu_all.finish()
    users((pc.mate_x, pc.mate_y, pc.dg, pc.mate_d))
    for h in range(2):
        egat[pc.r, h * D:(h + 1) * D, :] = eus[h].astype(BF16)
    ge.start()
    gq.wait_mate()
    diffs((pc.mate, pc.xn, pc.yn))
    gq.last()
    gq.wait_mates()
    diffs((pc.mate_x, pc.mate_y))
    gq.finish()
    diffs((pc.dg, pc.mate_d))
    swap = pc.to_z(dif, ur.at[1], zs.at[1, 0], zr.at[1, 0])
    mg[0] = pack_rows([jnp.sum(eus[h] * dif[h], axis=0, keepdims=True) for h in range(2)])
    mz = pc.to_z(mg.at[0], mg.at[1], zs.at[1, 4], zr.at[1, 4])
    mz.start()
    swap.start()
    ge.relay()
    acc = pi.at[1]
    acc[:6] = jnp.zeros((6, D, SHARD), F32)
    mz.wait()
    margin = mg[0] + mg[1]
    cg[pc.r, 0] = -jax.nn.sigmoid(-margin) / BATCH
    cg[pc.r, 1] = jnp.maximum(-margin, 0.0) + jnp.log1p(jnp.exp(-jnp.abs(margin)))
    coefs = []
    for j in range(1, ROWS):
        own = cg.at[pc.r]
        coefs.append(pc.to_row(own, own, ds.at[j - 1], dr.at[j - 1], (pc.r + j) % ROWS))
        coefs[-1].start()
    ge.last()
    two = 2 * USERS

    def lanes(q, h):
        return pl.ds(pl.multiple_of((q % 2) * two + h * USERS, USERS), USERS)

    def unit(q):
        return rd.at[0, q // 2, :, window(q % 2, two)]

    def unit_part(q, h):
        return rd.at[0, q // 2, h * HALF:(h + 1) * HALF, window(q % 2, two)]

    gv = Gather(pc, unit, unit_part, gs.at[4], gr.at[4])
    ge.wait_mate()
    ge.wait_mates()
    ge.finish()
    for cp in coefs:
        cp.wait()
    item_base = pc.c * ITEMS + pc.r * SHARD

    def item_grads(q, total):
        for h in range(2):
            k = q * 2 + h
            v = split3(unpack_row(cg[q, 0], h) * egat[q, h * D:(h + 1) * D, :].astype(F32))
            pos = named(1, k) - item_base
            neg = named(2, k) - item_base
            for n in range(0, SHARD, USERS):
                picks = [one_hot(pos - b, FOLD) - one_hot(neg - b, FOLD) for b in (n, n + FOLD)]
                part_g = lax.dot_general(v, jnp.concatenate(picks, axis=0), NT, preferred_element_type=F32)
                for j in range(3):
                    acc[j, :, n:n + USERS] += part_g[j * D:(j + 1) * D]
        return total + cg[q, 1]

    def user_grads(shards):
        def body(j, _):
            q, t = choose(j // 2, shards), j % 2
            w = split3(rd[0, q // 2, :, lanes(q, t)])
            for h in range(2):
                pick = one_hot(named(0, q * 2 + t) - (pc.r * 2 + h) * USERS, USERS)
                part_g = lax.dot_general(w, pick, NT, preferred_element_type=F32)
                for j in range(3):
                    acc[3 + j, :, h * USERS:(h + 1) * USERS] += part_g[j * D:(j + 1) * D]
            return 0

        lax.fori_loop(0, 2 * len(shards), body, 0)

    total = lax.fori_loop(0, 2, item_grads, jnp.zeros((ROWS, GROUP), F32))
    swap.wait()
    for h in range(2):
        rd[0, pc.r // 2, :, lanes(pc.r, h)] = unpack_row(cg[pc.r, 0], h) * (dif[h] + ur[1, h])
    gv.start()
    total = lax.fori_loop(2, 6, item_grads, total)
    gv.relay()
    total = lax.fori_loop(6, ROWS, item_grads, total)
    whole = jnp.sum(jnp.sum(total, axis=0, keepdims=True), axis=1, keepdims=True)
    loss[...] = whole / BATCH
    src_i, src_u = acci, accu
    src_i[...] = ((acc[0] + acc[1]) + acc[2]) / (LAYERS + 1)
    gv.wait_mate()

    objs['xis'], objs['gath'] = objs['xis'][::-1], objs['gath'][::-1]
    gp, gq = objs['gath']
    xi1[pc.r] = src_i[...].astype(BF16)
    gp.start()
    user_grads((pc.r, pc.mate, pc.xn, pc.yn))
    gv.last()
    gv.wait_mates()
    user_grads((pc.mate_x, pc.mate_y))
    gv.finish()
    user_grads((pc.dg, pc.mate_d))
    for h in range(2):
        there = slice(h * USERS, (h + 1) * USERS)
        src_u[h] = ((acc[3, :, there] + acc[4, :, there]) + acc[5, :, there]) / (LAYERS + 1)
        xu[0, h] = src_u[h].astype(BF16)

    def back_u(k, h, total):
        value = src_u[h] + total
        if k == LAYERS:
            @pl.when(pc.c == h)
            def _():
                gu[...] = value
        return value.astype(BF16)

    def back_i(k, rows, total):
        value = src_i[rows] + total
        if k == LAYERS:
            gi[rows] = value
        return value.astype(BF16)

    propagate(fin_u=back_u, fin_i=back_i, gather_first=True, **objs)


def mega_call(mask_blk, u0, i0, ids):
    dma = pltpu.SemaphoreType.DMA
    vm = pl.BlockSpec(memory_space=pltpu.VMEM)
    hbm = pl.BlockSpec(memory_space=pl.ANY)
    i32 = jnp.int32
    shape = jax.ShapeDtypeStruct
    return pl.pallas_call(
        mega_kernel,
        name='mega',
        out_shape=(shape((D, USERS), BF16), shape((D, SHARD), BF16), shape((1, 1), F32), shape((D, USERS), F32), shape((D, SHARD), F32)),
        in_specs=[hbm, vm, vm, vm],
        out_specs=(vm, vm, vm, vm, vm),
        scratch_shapes=comm_scratch() + [
            pltpu.VMEM((ROWS, ROWS, FOLD), i32),
            pltpu.VMEM((ROWS - 1, ROWS, ROWS, FOLD), i32),
            pltpu.VMEM((ROWS, 2 * USERS), i32),
            pltpu.VMEM((ROWS, 2 * USERS), i32),
            pltpu.VMEM((TWO, D, USERS), F32),
            pltpu.VMEM((D, SHARD), F32),
            pltpu.VMEM((ROWS, 2 * D, USERS), BF16),
            pltpu.VMEM((ROWS, 2 * D, USERS), BF16),
            pltpu.VMEM((ROWS, TWO, ROWS, GROUP), F32),
            pltpu.VMEM((TWO, ROWS, GROUP), F32),
            dma((ROWS,)), dma((ROWS,)),
        ],
        compiler_params=pltpu.CompilerParams(collective_id=0, has_side_effects=True, vmem_limit_bytes=VMEM_LIMIT),
    )(mask_blk, u0, i0, ids)


def settle_kernel(*refs):
    half = len(refs) // 2
    for src, dst in zip(refs[:half], refs[half:]):
        dst[...] = src[...]


def settle_call(*arrays):
    shapes = tuple(jax.ShapeDtypeStruct(x.shape, x.dtype) for x in arrays)
    return pl.pallas_call(settle_kernel, name='settle', out_shape=shapes)(*arrays)


def solution(mesh):
    def local_fn(mask_blk, user_emb, item_emb, triples):
        eu, ei, loss, gu, gi = settle_call(*mega_call(mask_blk, user_emb.T, item_emb.T, triples.T))
        return eu.T, ei.T, loss.reshape(()), gu.T, gi.T

    user_spec = P(('row', 'col'), None)
    item_spec = P(('col', 'row'), None)
    return jax.shard_map(local_fn, mesh=mesh, in_specs=(P('row', 'col'), user_spec, item_spec, P()), out_specs=(user_spec, item_spec, P(), user_spec, item_spec), check_vma=False)
```
